256 devices in a mesh: rows: 32 (over y, x, core), feat: 8 (over z).
Axes of the slice: x: 4, y: 4, z: 8, core: 2. Of those that a mesh axis runs over, the one named last changes fastest.
Arguments:
- features: bfloat16 [32768, 2048], P('rows', 'feat'), may hold values from -6 to 6
- grad_out: bfloat16 [32768, 2048], P('rows', 'feat'), may hold values from -6 to 6
- eigvecs: float32 [2048, 2048], P('feat', 'rows'), may hold values from -1 to 1, as said below
- eigvals: float32 [2048], replicated, may hold values from 0.1 to 1, as said below
- whiten: bfloat16 [2048, 2048], P(None, 'feat'), may hold values from -0.125 to 0.125
Outputs:
- grad_in: bfloat16 [32768, 2048], P('rows', 'feat')
The draws below stay inside these ranges and needn't reach their ends.
Inputs may be any that keep to these rules, and one draw needn't show every extreme that they name: `eigvecs`: the columns are orthonormal. `eigvals`: any two entries differ by at least 0.45 / 2048.
All inputs are finite; a program needn't handle non-finite values.
Results may differ from the reference program's by a relative error of at most 0.0074.
Values may be sent and summed in bfloat16 or wider, within the bound.
A program may use at most 128 MiB of HBM per device.

```python
import jax
import jax.numpy as jnp
from jax import lax

D = 2048
TOKENS = 32768


def draw_eigvecs(key, part):
    normal_mat = jax.random.normal(key, (D, D), jnp.float32)
    ortho, upper = jnp.linalg.qr(normal_mat)
    return ortho


def draw_eigvals(key, part):
    ranking = jax.random.permutation(jax.random.fold_in(key, 1), D)
    jitter = jax.random.uniform(jax.random.fold_in(key, 2), (D,), jnp.float32)
    return 0.1 + 0.9 * (ranking.astype(jnp.float32) + 0.25 + 0.5 * jitter) / D


def block_levels(own_key, extent, shards, low, top_value):
    loudness, own = 1.0, jax.random.fold_in(own_key, 6)
    for dim, parts in shards:
        heights = jnp.exp(jax.random.uniform(jax.random.fold_in(own, dim), (parts,), jnp.float32, low / len(shards), top_value / len(shards)))
        loudness = loudness * jnp.repeat(heights, extent[dim] // parts).reshape([-1 if axis == dim else 1 for axis in range(len(extent))])
    return loudness


def gaussian(own_key, extent, width, bound, split=(), held_as=jnp.bfloat16):
    entries = width * jax.random.normal(own_key, extent, jnp.float32)
    if split:
        entries = entries * block_levels(own_key, extent, split, -0.22, 0.18)
    return jnp.clip(entries, -bound, bound).astype(held_as)


def setup_inputs(seed: int = 0) -> dict:
    keys = jax.random.split(jax.random.key(seed), 6)
    return {
        "features": gaussian(keys[0], (TOKENS, D), 1.0, 6.0, ((0, 32), (1, 8))),
        "grad_out": gaussian(keys[1], (TOKENS, D), 1.0, 6.0, ((0, 32), (1, 8))),
        "eigvecs": draw_eigvecs(jax.random.fold_in(keys[5], 71), 0),
        "eigvals": draw_eigvals(jax.random.fold_in(keys[5], 71), 0),
        "whiten": gaussian(keys[4], (D, D), D ** -0.5, 0.125, ((1, 8),)),
    }


def divided(lam_row, lam_col, first_col):
    on_diag = jnp.arange(lam_row.shape[0], dtype=jnp.int32)[:, None] == (first_col + jnp.arange(lam_col.shape[0], dtype=jnp.int32))[None, :]
    root_row = lam_row ** (-0.5)
    root_col = lam_col ** (-0.5)
    gaps_lam = lam_row[:, None] - lam_col[None, :]
    safe_gap = jnp.where(on_diag, jnp.ones_like(gaps_lam), gaps_lam)
    off_diag = (root_row[:, None] - root_col[None, :]) / safe_gap
    diag_vals = -0.5 * lam_row[:, None] ** (-1.5) + jnp.zeros_like(gaps_lam)
    return jnp.where(on_diag, diag_vals, off_diag)

def reference(features, grad_out, eigvecs, eigvals, whiten):
    highest = lax.Precision.HIGHEST
    row_count = features.shape[0]
    col_mean = jnp.sum(features.astype(jnp.float32), axis=0) / row_count
    grad_mean = jnp.sum(grad_out.astype(jnp.float32), axis=0) / row_count
    cross_prod = jnp.dot(features.T.astype(jnp.float32), grad_out.astype(jnp.float32), preferred_element_type=jnp.float32) - row_count * jnp.outer(col_mean, grad_mean)
    sym_gram = 0.5 * (cross_prod + cross_prod.T)
    rotated = jnp.dot(eigvecs.T, jnp.dot(sym_gram, eigvecs, precision=highest), precision=highest)
    kernel = divided(eigvals, eigvals, 0)
    sens = jnp.dot(jnp.dot(eigvecs, kernel * rotated, precision=highest), eigvecs.T, precision=highest)
    sens_scaled = (2.0 / row_count * sens).astype(jnp.bfloat16)
    shifted = (grad_out.astype(jnp.float32) - grad_mean).astype(jnp.bfloat16)
    centered = (features.astype(jnp.float32) - col_mean).astype(jnp.bfloat16)
    grad_in = jnp.dot(shifted.astype(jnp.float32), whiten.astype(jnp.float32), preferred_element_type=jnp.float32) + jnp.dot(centered.astype(jnp.float32), sens_scaled.T.astype(jnp.float32), preferred_element_type=jnp.float32)
    return grad_in.astype(jnp.bfloat16)
```

```python
import functools
import math

import jax
import jax.numpy as jnp
from jax import lax
from jax.experimental import pallas as pl
from jax.experimental.pallas import tpu as pltpu
from jax.sharding import PartitionSpec as P

MESH = pl.DeviceIdType.MESH
VMEM = pl.BlockSpec(memory_space=pltpu.VMEM)
bf16, f32 = jnp.bfloat16, jnp.float32
CHUNKS = 4


def remote(src, dst, send, recv, axis, target):
    return pltpu.make_async_remote_copy(
        src_ref=src, dst_ref=dst, send_sem=send, recv_sem=recv,
        device_id={axis: target}, device_id_type=MESH,
    )


def lanes(index, width):
    return pl.ds(pl.multiple_of(index * width, width), width)


def mm(a, b, ca=1, cb=0):
    return lax.dot_general(a, b, (((ca,), (cb,)), ((), ())), preferred_element_type=f32)


def slot_order(zn):
    order = [0]
    for dist in range(1, zn // 2):
        order += [zn - dist, dist]
    return order + [zn // 2]


def body(n, zn, row_count, x_ref, g_ref, v_ref, k_ref, w_ref, o_ref,
         x_all, g_all, v_all, v_pair, xct, gc, acc, sums, sums_own, means, pieces, parts, tot, tile, rtile, spiece, sall,
         vct, yacc, yown, yall, mt, town, tall,
         ring_s, ring_r, vr_s, vr_r, vm_s, vm_r, v1_s, v1_r, v2_s, v2_r, vd_s, vd_r, su_s, su_r, me_s, me_r,
         rs_s, rs_r, sy_s, sy_r, ag_s, ag_r, am_s, am_r, ya_s, ya_r):
    me, z = lax.axis_index("rows"), lax.axis_index("feat")
    core, chip = lax.rem(me, 2), me // 2
    mate = me + 1 - 2 * core
    h = n // 2
    nx = math.isqrt(h)
    ny = h // nx
    yy, xx = chip // nx, lax.rem(chip, nx)
    half = zn // 2
    tok, own = x_ref.shape
    nar = k_ref.shape[0]
    wide = 2 * nar
    hv = own // 2
    rp = own // n
    ck = tok // CHUNKS
    order = slot_order(zn)
    every = list(range(CHUNKS))
    pending = []

    barrier = pltpu.get_barrier_semaphore()
    for d in range(1, n):
        pl.semaphore_signal(barrier, inc=1, device_id={"rows": lax.rem(me + d, n)}, device_id_type=MESH)
    for d in range(1, zn):
        pl.semaphore_signal(barrier, inc=1, device_id={"feat": lax.rem(z + d, zn)}, device_id_type=MESH)
    pl.semaphore_wait(barrier, n + zn - 2)

    def at_z(rel):
        return lax.rem(z + rel, zn)

    def block_of(way, dist):
        return at_z(zn - dist) if way == 0 else at_z(dist)

    def next_of(way):
        return at_z(1) if way == 0 else at_z(zn - 1)

    def units(step, way):
        if step < half - 1:
            return every
        return every[: CHUNKS // 2] if way == 0 else every[CHUNKS // 2:]

    def hop(arr, way, step, unit):
        full, mine = (g_all, g_ref) if arr == 0 else (x_all, x_ref)
        there = full.at[block_of(way, step), pl.ds(unit * ck, ck)]
        src = there if step else mine.at[pl.ds(unit * ck, ck)]
        return remote(src, there, ring_s.at[arr, way, step, unit], ring_r.at[arr, way, step, unit], "feat", next_of(way))

    def vpart(block, rows_half, lane, count=1):
        start = pl.multiple_of(block * own + rows_half * hv, hv)
        return v_all.at[pl.ds(start, hv), pl.ds(pl.multiple_of(lane * wide, wide), wide * count)]

    def vhop(way, step):
        ref = vpart(block_of(way, step), core, chip)
        return remote(ref, ref, vr_s.at[way, step], vr_r.at[way, step], "feat", next_of(way))

    def y_first(rel):
        return rel == 0 or rel > half

    def v_one(rel, d):
        ref = vpart(at_z(rel), core, chip)
        if y_first(rel):
            target = (lax.rem(yy + d, ny) * nx + xx) * 2 + core
        else:
            target = (yy * nx + lax.rem(xx + d, nx)) * 2 + core
        return remote(ref, ref, v1_s.at[rel, d - 1], v1_r.at[rel, d - 1], "rows", target)

    def v_two(rel):
        copies = []
        if y_first(rel):
            for e in range(ny):
                ref = vpart(at_z(rel), core, lax.rem(yy + ny - e, ny) * nx + xx)
                for d in range(1, nx):
                    i = e * (nx - 1) + d - 1
                    target = (yy * nx + lax.rem(xx + d, nx)) * 2 + core
                    copies.append(remote(ref, ref, v2_s.at[rel, i], v2_r.at[rel, i], "rows", target))
        else:
            start = pl.multiple_of(at_z(rel) * own + core * hv, hv)
            ref = v_all.at[pl.ds(start, hv), lanes(yy, nx * wide)]
            for d in range(1, ny):
                target = (lax.rem(yy + d, ny) * nx + xx) * 2 + core
                copies.append(remote(ref, ref, v2_s.at[rel, d - 1], v2_r.at[rel, d - 1], "rows", target))
        return copies

    def ones(rel):
        return range(1, ny if y_first(rel) else nx)

    def v_start(rel):
        for d in ones(rel):
            v_one(rel, d).start()

    def v_second(rel):
        for d in ones(rel):
            v_one(rel, d).wait_recv()
        for copy in v_two(rel):
            copy.start()

    def v_mate(rel):
        start = pl.multiple_of(at_z(rel) * own + core * hv, hv)
        ref = v_all.at[pl.ds(start, hv)]
        return remote(ref, ref, vd_s.at[rel], vd_r.at[rel], "rows", mate)

    def v_third(rel):
        for copy in v_two(rel):
            copy.wait_recv()
        v_mate(rel).start()

    for way in (0, 1):
        hop(0, way, 0, units(0, way)[0]).start()
    v_pair[core] = v_ref[...].astype(bf16)
    pair = remote(v_pair.at[core], v_pair.at[core], vm_s.at[0], vm_r.at[0], "rows", mate)
    pair.start()
    sums_own[...] = jnp.zeros_like(sums_own)
    sums_own[0:1] = jnp.sum(x_ref[...].astype(f32), axis=0, keepdims=True)
    sums_own[1:2] = jnp.sum(g_ref[...].astype(f32), axis=0, keepdims=True)
    pair.wait_recv()
    v_all[pl.ds(pl.multiple_of(z * own, own), own), lanes(chip, wide)] = jnp.concatenate([v_pair[0], v_pair[1]], axis=1)
    for way in (0, 1):
        if way == 0 or half > 1:
            vhop(way, 0).start()
        for unit in units(0, way)[1:]:
            hop(0, way, 0, unit).start()
    sum_copies = []
    for d in range(1, n):
        copy = remote(sums_own, sums.at[me], su_s.at[d - 1], su_r.at[d - 1], "rows", lax.rem(me + d, n))
        copy.start()
        sum_copies.append(copy)
    sums[me] = sums_own[...]
    pending += sum_copies + [pair]
    v_start(0)
    x_all[z] = x_ref[...]
    for copy in sum_copies:
        copy.wait_recv()
    means[z] = jnp.sum(sums[...], axis=0) / row_count
    mean_copies = []
    for d in range(1, zn):
        copy = remote(means.at[z], means.at[z], me_s.at[d - 1], me_r.at[d - 1], "feat", at_z(d))
        copy.start()
        mean_copies.append(copy)
    pending += mean_copies
    xc = (x_ref[...].astype(f32) - means[z, 0:1]).astype(bf16)
    xct[...] = xc.astype(f32).T.astype(bf16)

    def gram(slot):
        rel = order[slot]
        q = at_z(rel)
        src = g_ref if rel == 0 else g_all.at[q]
        gc[...] = (src[...].astype(f32) - means[q, 1:2]).astype(bf16)
        block = mm(xct[...], gc[...])
        lane = pl.ds(slot * own, own)

        def put(value):
            pieces[:, :, lane] = value.reshape(n, rp, own).astype(bf16)

        if rel == 0:
            put(0.5 * (block + block.T))
        else:
            @pl.when(z < q)
            def _():
                put(0.5 * block)

            @pl.when(z > q)
            def _():
                put(0.5 * block.T)
        gw = mm(gc[...], w_ref[pl.ds(pl.multiple_of(q * own, own), own)])
        acc[...] = gw if slot == 0 else acc[...] + gw

    split = max(1, zn - 3)
    groups = [(0, split), (split, zn)]

    def rs(group, d):
        lo, hi = groups[group]
        lane = pl.ds(lo * own, (hi - lo) * own)
        s = lax.rem(me + d, n)
        return remote(pieces.at[s, :, lane], parts.at[me, :, lane], rs_s.at[group, d - 1], rs_r.at[group, d - 1], "rows", s)

    def rs_start(group):
        for d in range(1, n):
            rs(group, d).start()

    def rs_sum(group):
        lo, hi = groups[group]
        lane = pl.ds(lo * own, (hi - lo) * own)
        total = pieces[me, :, lane].astype(f32)
        for d in range(1, n):
            rs(group, d).wait_recv()
            total = total + parts[lax.rem(me + n - d, n), :, lane].astype(f32)
        for slot in range(lo, hi):
            tile[slot] = total[:, (slot - lo) * own:(slot - lo + 1) * own].astype(bf16)

    gram(0)
    rels = [[0]]
    started = False
    first_wait = True
    for dist in range(1, half + 1):
        got = []
        for way in (0, 1):
            if way == 0 or dist < half:
                vhop(way, dist - 1).wait_recv()
                if (way == 0 and dist < half) or (way == 1 and dist < half - 1):
                    vhop(way, dist).start()
                rel = zn - dist if way == 0 else dist
                v_start(rel)
                got.append(rel)
        rels.append(got)
        if dist == half and zn > 2:
            pass
        for unit in every:
            for way in (0, 1):
                if unit in units(dist - 1, way):
                    hop(0, way, dist - 1, unit).wait_recv()
                    if dist < half and unit in units(dist, way):
                        hop(0, way, dist, unit).start()
        if dist == half - 1 or half == 1:
            for unit in every:
                for way in (0, 1):
                    if unit in units(0, way):
                        hop(1, way, 0, unit).start()
        for rel in rels[dist - 1]:
            v_second(rel)
        if dist >= 2:
            for rel in rels[dist - 2]:
                v_third(rel)
        if first_wait:
            for copy in mean_copies:
                copy.wait_recv()
            first_wait = False
        for slot in range(zn):
            if order[slot] in (dist, zn - dist):
                gram(slot)
                if slot == split - 1:
                    rs_start(0)
        if split == 1 and dist == 1:
            rs_start(0)
    rs_start(1)
    for rel in rels[half]:
        v_second(rel)
    for rel in rels[half - 1]:
        v_third(rel)

    forwards = [(step, unit) for step in range(1, half) for unit in every]
    state = {"next": 0}

    def pump(count):
        for _ in range(count):
            if state["next"] < len(forwards):
                step, unit = forwards[state["next"]]
                state["next"] += 1
                for way in (0, 1):
                    if unit in units(step - 1, way):
                        hop(1, way, step - 1, unit).wait_recv()
                        if unit in units(step, way):
                            hop(1, way, step, unit).start()

    rs_sum(0)
    rs_sum(1)

    sym = []
    for slot in range(1, zn):
        d = order[slot]
        copy = remote(tile.at[slot], rtile.at[order.index((zn - d) % zn)], sy_s.at[d - 1], sy_r.at[d - 1], "feat", at_z(d))
        copy.start()
        sym.append(copy)
    pending += sym
    for rel in rels[half]:
        v_third(rel)
    pump(2)
    for copy in sym:
        copy.wait_recv()
    spiece[:, pl.ds(0, own)] = tile[0]
    for slot in range(1, zn):
        both = tile[slot].astype(f32) + rtile[slot].astype(f32)
        spiece[:, pl.ds(slot * own, own)] = both.astype(bf16)

    def gather_start(which, src, full):
        copies = []
        for d in range(1, h):
            copy = remote(src, full.at[me], ag_s.at[which, d], ag_r.at[which, d], "rows", lax.rem(me + 2 * d, n))
            copy.start()
            copies.append(copy)
        passed = remote(src, full.at[me], am_s.at[which, 0], am_r.at[which, 0], "rows", mate)
        passed.start()
        full[me] = src[...]
        return copies, [passed]

    def gather_end(which, full, copies, passed):
        for d in range(1, h):
            source = lax.rem(me + n - 2 * d, n)
            copies[d - 1].wait_recv()
            copy = remote(full.at[source], full.at[source], am_s.at[which, d], am_r.at[which, d], "rows", mate)
            copy.start()
            passed.append(copy)
        for copy in passed:
            copy.wait_recv()
        return copies + passed

    copies, passed = gather_start(0, spiece, sall)
    for rel in range(zn):
        v_mate(rel).wait_recv()
    vct[...] = v_all[:, lanes(chip, wide)].astype(f32).T.astype(bf16)
    pump(2)
    pending += gather_end(0, sall, copies, passed)

    yacc[...] = jnp.zeros_like(yacc)
    own_rows = pl.ds(pl.multiple_of(core * nar, nar), nar)
    for slot in range(zn):
        q = at_z(order[slot])
        block = sall[:, :, pl.ds(slot * own, own)].astype(f32).reshape(own, own).astype(bf16)
        left = vct[own_rows, lanes(q, own)]
        if slot == 0:
            yacc[...] += mm(left, block)
        else:
            @pl.when(q < z)
            def _():
                yacc[...] += mm(left, block)

            @pl.when(q > z)
            def _():
                yacc[...] += mm(left, block, 1, 1)
    yown[...] = yacc[...].astype(bf16)
    ysend = []
    for d in range(1, zn):
        copy = remote(yown, yall.at[z], ya_s.at[d - 1], ya_r.at[d - 1], "feat", at_z(d))
        copy.start()
        ysend.append(copy)
    pending += ysend
    yall[z] = yown[...]
    pump(2)
    for copy in ysend:
        copy.wait_recv()
    d_all = v_all.shape[0]
    left = jnp.concatenate([yall[q] for q in range(zn)], axis=1)
    mt[...] = (k_ref[...] * mm(left, v_all[...])).astype(bf16)
    town[...] = mm(mt[...], v_all[pl.ds(pl.multiple_of(z * own, own), own)], 1, 1).astype(bf16)
    copies, passed = gather_start(1, town, tall)
    pump(len(forwards))
    pending += gather_end(1, tall, copies, passed)
    for way in (0, 1):
        for unit in units(half - 1, way):
            hop(1, way, half - 1, unit).wait_recv()

    @pl.loop(0, zn)
    def _(q):
        sens = mm(v_all[pl.ds(pl.multiple_of(q * own, own), own)], tall[...].reshape(d_all, own))
        sens = ((2.0 / row_count) * sens).astype(bf16)
        xq = (x_all[q].astype(f32) - means[q, 0:1]).astype(bf16)
        acc[...] += mm(xq, sens)

    o_ref[...] = acc[...].astype(bf16)

    for copy in pending:
        copy.wait_send()
    for group in range(2):
        for d in range(1, n):
            rs(group, d).wait_send()
    for arr in (0, 1):
        for way in (0, 1):
            for step in range(half):
                for unit in units(step, way):
                    hop(arr, way, step, unit).wait_send()
    for step in range(half):
        for way in (0, 1):
            if way == 0 or step < half - 1:
                vhop(way, step).wait_send()
    for rel in range(zn):
        for d in ones(rel):
            v_one(rel, d).wait_send()
        for copy in v_two(rel):
            copy.wait_send()
        v_mate(rel).wait_send()


def divided(lam_row, lam_col, first_row):
    on_diag = (
        (first_row + jnp.arange(lam_row.shape[0], dtype=jnp.int32))[:, None]
        == jnp.arange(lam_col.shape[0], dtype=jnp.int32)[None, :]
    )
    root_row = lam_row ** (-0.5)
    root_col = lam_col ** (-0.5)
    gaps_lam = lam_row[:, None] - lam_col[None, :]
    safe_gap = jnp.where(on_diag, jnp.ones_like(gaps_lam), gaps_lam)
    off_diag = (root_row[:, None] - root_col[None, :]) / safe_gap
    diag_vals = -0.5 * lam_row[:, None] ** (-1.5) + jnp.zeros_like(gaps_lam)
    return jnp.where(on_diag, diag_vals, off_diag)


def local(features, grad_out, eigvecs, eigvals, whiten):
    tok, own = features.shape
    n, zn = lax.axis_size("rows"), lax.axis_size("feat")
    d_all = eigvals.shape[0]
    nar, rp = d_all // n, own // n
    h, half = n // 2, zn // 2
    nx = math.isqrt(h)
    row_count = tok * n
    first = lax.axis_index("rows") * nar
    kernel_rows = divided(lax.dynamic_slice_in_dim(eigvals, first, nar), eigvals, first)
    scratch = [
        pltpu.VMEM((zn, tok, own), bf16),
        pltpu.VMEM((zn, tok, own), bf16),
        pltpu.VMEM((d_all, d_all), bf16),
        pltpu.VMEM((2, own, nar), bf16),
        pltpu.VMEM((own, tok), bf16),
        pltpu.VMEM((tok, own), bf16),
        pltpu.VMEM((tok, own), f32),
        pltpu.VMEM((n, 8, own), f32),
        pltpu.VMEM((8, own), f32),
        pltpu.VMEM((zn, 8, own), f32),
        pltpu.VMEM((n, rp, d_all), bf16),
        pltpu.VMEM((n, rp, d_all), bf16),
        pltpu.VMEM((8, 128), f32),
        pltpu.VMEM((zn, rp, own), bf16),
        pltpu.VMEM((zn, rp, own), bf16),
        pltpu.VMEM((rp, d_all), bf16),
        pltpu.VMEM((n, rp, d_all), bf16),
        pltpu.VMEM((2 * nar, d_all), bf16),
        pltpu.VMEM((nar, own), f32),
        pltpu.VMEM((nar, own), bf16),
        pltpu.VMEM((zn, nar, own), bf16),
        pltpu.VMEM((nar, d_all), bf16),
        pltpu.VMEM((nar, own), bf16),
        pltpu.VMEM((n, nar, own), bf16),
    ]

    def sems(*shape):
        return [pltpu.SemaphoreType.DMA(shape)] * 2

    scratch += sems(2, 2, half, CHUNKS) + sems(2, half) + sems(1) + sems(zn, nx) + sems(zn, nx * nx) + sems(zn)
    scratch += sems(n - 1) + sems(zn - 1) + sems(2, n - 1) + sems(zn - 1) + sems(2, h) + sems(2, h) + sems(zn - 1)
    return pl.pallas_call(
        functools.partial(body, n, zn, row_count),
        out_shape=jax.ShapeDtypeStruct((tok, own), bf16),
        in_specs=[VMEM] * 5,
        out_specs=VMEM,
        scratch_shapes=scratch,
        compiler_params=pltpu.CompilerParams(collective_id=1, has_side_effects=True, vmem_limit_bytes=58 * 2**20),
        cost_estimate=pl.CostEstimate(flops=8_000_000_000, bytes_accessed=16 * 2**20, transcendentals=0),
    )(features, grad_out, eigvecs, kernel_rows, whiten)


def solution(mesh):
    in_specs = (P("rows", "feat"), P("rows", "feat"), P("feat", "rows"), P(), P(None, "feat"))
    out_specs = P("rows", "feat")
    return jax.shard_map(local, mesh=mesh, in_specs=in_specs, out_specs=out_specs, check_vma=False)
```

```python
import functools
import math

import jax
import jax.numpy as jnp
from jax import lax
from jax.experimental import pallas as pl
from jax.experimental.pallas import tpu as pltpu
from jax.sharding import PartitionSpec as P

MESH = pl.DeviceIdType.MESH
VMEM = pl.BlockSpec(memory_space=pltpu.VMEM)
bf16, f32 = jnp.bfloat16, jnp.float32
CHUNKS = 4


def remote(src, dst, send, recv, axis, target):
    return pltpu.make_async_remote_copy(
        src_ref=src, dst_ref=dst, send_sem=send, recv_sem=recv,
        device_id={axis: target}, device_id_type=MESH,
    )


def lanes(index, width):
    return pl.ds(pl.multiple_of(index * width, width), width)


def mm(a, b, ca=1, cb=0):
    return lax.dot_general(a, b, (((ca,), (cb,)), ((), ())), preferred_element_type=f32)


def slot_order(zn):
    order = [0]
    for dist in range(1, zn // 2):
        order += [zn - dist, dist]
    return order + [zn // 2]


def body(n, zn, row_count, x_hbm, g_hbm, v_hbm, e_hbm, w_hbm, o_ref,
         x_ref, g_ref, v_ref, e_ref, w_ref, x_all, xc_all, g_all, v_all, v_pair, xct, gc, acc, sums, sums_own, means,
         pieces, parts, tile, rtile, spiece, sall, vct, yacc, yown, yall, kern, mt, town, tall, sens,
         ld, ring_s, ring_r, vr_s, vr_r, vm, v1_s, v1_r, v2_s, v2_r, vd, su, me_sem, rs_sem, sy_sem, ag_sem, am_sem, ya_sem):
    me, z = lax.axis_index("rows"), lax.axis_index("feat")
    core, chip = lax.rem(me, 2), me // 2
    mate = me + 1 - 2 * core
    h = n // 2
    nx = math.isqrt(h)
    ny = h // nx
    yy, xx = chip // nx, lax.rem(chip, nx)
    half = zn // 2
    tok, own = x_ref.shape
    d_all = v_all.shape[0]
    nar = d_all // n
    wide = 2 * nar
    hv = own // 2
    rp = own // n
    ck = tok // CHUNKS
    order = slot_order(zn)
    every = list(range(CHUNKS))
    loads = []
    for i, (src, dst) in enumerate([(g_hbm, g_ref), (v_hbm, v_ref), (x_hbm, x_ref), (e_hbm, e_ref), (w_hbm, w_ref)]):
        load = pltpu.make_async_copy(src, dst, ld.at[i])
        load.start()
        loads.append(load)
    barrier = pltpu.get_barrier_semaphore()
    for d in range(1, n):
        pl.semaphore_signal(barrier, inc=1, device_id={"rows": lax.rem(me + d, n)}, device_id_type=MESH)
    for d in range(1, zn):
        pl.semaphore_signal(barrier, inc=1, device_id={"feat": lax.rem(z + d, zn)}, device_id_type=MESH)
    loads[0].wait()
    loads[1].wait()
    v_pair[core] = v_ref[...].astype(bf16)
    pl.semaphore_wait(barrier, n + zn - 2)

    def at_z(rel):
        return lax.rem(z + rel, zn)

    def rows_of(block, count):
        return pl.ds(pl.multiple_of(block * count, count), count)

    def arrived(ref, sem):
        pltpu.make_async_copy(ref, ref, sem).wait()

    def block_of(way, dist):
        return at_z(zn - dist) if way == 0 else at_z(dist)

    def next_of(way):
        return at_z(1) if way == 0 else at_z(zn - 1)

    def units(step, way):
        if step < half - 1:
            return every
        return every[: CHUNKS // 2] if way == 0 else every[CHUNKS // 2:]

    def hop(arr, way, step, unit):
        full, mine = (g_all, g_ref) if arr == 0 else (x_all, x_ref)
        there = full.at[block_of(way, step), pl.ds(unit * ck, ck)]
        src = there if step else mine.at[pl.ds(unit * ck, ck)]
        return remote(src, there, ring_s.at[arr], ring_r.at[arr, way, step, unit], "feat", next_of(way))

    def vpart(block, lane):
        return v_all.at[rows_of(2 * block + core, hv), lanes(lane, wide)]

    def v_arrived(count, sem):
        if count * wide > d_all:
            arrived(v_all.at[pl.ds(0, count * wide * hv // d_all)], sem)
        elif count:
            arrived(v_all.at[pl.ds(0, hv), pl.ds(0, count * wide)], sem)

    def vhop(way, step):
        ref = vpart(block_of(way, step), chip)
        return remote(ref, ref, vr_s.at[0], vr_r.at[way, step], "feat", next_of(way))

    def y_first(rel):
        return rel == 0 or rel > half

    def by_y(d):
        return (lax.rem(yy + d, ny) * nx + xx) * 2 + core

    def by_x(d):
        return (yy * nx + lax.rem(xx + d, nx)) * 2 + core

    def v_first(rel):
        ref = vpart(at_z(rel), chip)
        for d in range(1, ny if y_first(rel) else nx):
            target = by_y(d) if y_first(rel) else by_x(d)
            remote(ref, ref, v1_s.at[0], v1_r.at[rel], "rows", target).start()

    def v_second(rel):
        v_arrived((ny if y_first(rel) else nx) - 1, v1_r.at[rel])
        if y_first(rel):
            for e in range(ny):
                ref = vpart(at_z(rel), lax.rem(yy + ny - e, ny) * nx + xx)
                for d in range(1, nx):
                    remote(ref, ref, v2_s.at[0], v2_r.at[rel], "rows", by_x(d)).start()
        else:
            ref = v_all.at[rows_of(2 * at_z(rel) + core, hv), lanes(yy, nx * wide)]
            for d in range(1, ny):
                remote(ref, ref, v2_s.at[0], v2_r.at[rel], "rows", by_y(d)).start()

    def v_third(rel):
        v_arrived(ny * (nx - 1) if y_first(rel) else nx * (ny - 1), v2_r.at[rel])
        ref = v_all.at[rows_of(2 * at_z(rel) + core, hv)]
        remote(ref, ref, vd.at[0], vd.at[1], "rows", mate).start()
    for way in (0, 1):
        hop(0, way, 0, units(0, way)[0]).start()
    pair = remote(v_pair.at[core], v_pair.at[core], vm.at[0], vm.at[1], "rows", mate)
    pair.start()
    loads[2].wait()
    sums_own[...] = jnp.zeros_like(sums_own)
    sums_own[0:1] = jnp.sum(x_ref[...].astype(f32), axis=0, keepdims=True)
    sums_own[1:2] = jnp.sum(g_ref[...].astype(f32), axis=0, keepdims=True)
    pair.wait_recv()
    both = jnp.concatenate([v_pair[0].astype(f32), v_pair[1].astype(f32)], axis=0)
    v_all[rows_of(z, own), lanes(chip, wide)] = both.T.astype(bf16)
    for way in (0, 1):
        if way == 0 or half > 1:
            vhop(way, 0).start()
        for unit in units(0, way)[1:]:
            hop(0, way, 0, unit).start()
    for d in range(1, n):
        remote(sums_own, sums.at[me], su.at[0], su.at[1], "rows", lax.rem(me + d, n)).start()
    sums[me] = sums_own[...]
    v_first(0)
    loads[3].wait()
    root = jnp.sqrt(e_ref[...])
    shape = (nar, d_all)
    wanted = me * nar + lax.broadcasted_iota(jnp.int32, shape, 0)
    hit = wanted == lax.broadcasted_iota(jnp.int32, shape, 1)
    root_row = jnp.sum(jnp.where(hit, jnp.broadcast_to(root, shape), 0.0), axis=1, keepdims=True)
    kern[...] = -1.0 / ((root_row * root) * (root_row + root))
    arrived(sums.at[pl.ds(0, n - 1)], su.at[1])
    means[z] = jnp.sum(sums[...], axis=0) / row_count
    for d in range(1, zn):
        remote(means.at[z], means.at[z], me_sem.at[0], me_sem.at[1], "feat", at_z(d)).start()
    xc = x_ref[...].astype(f32) - means[z, 0:1]
    xc_all[z] = xc.astype(bf16)
    xct[...] = xc.T.astype(bf16)
    loads[4].wait()

    def gram(slot):
        rel = order[slot]
        q = at_z(rel)
        src = g_ref if rel == 0 else g_all.at[q]
        gc[...] = (src[...].astype(f32) - means[q, 1:2]).astype(bf16)
        block = mm(xct[...], gc[...])
        lane = pl.ds(slot * own, own)

        def put(value):
            pieces[:, :, lane] = value.reshape(n, rp, own).astype(bf16)

        if rel == 0:
            put(0.5 * (block + block.T))
        else:
            @pl.when(z < q)
            def _():
                put(0.5 * block)

            @pl.when(z > q)
            def _():
                put(0.5 * block.T)

    def product(slot):
        gw = mm(gc[...], w_ref[rows_of(at_z(order[slot]), own)])
        acc[...] = gw if slot == 0 else acc[...] + gw

    split = max(1, zn - 3)
    groups = [(0, split), (split, zn)]
    group_lanes = [pl.ds(lo * own, (hi - lo) * own) for lo, hi in groups]

    def rs_start(group):
        lane = group_lanes[group]
        for d in range(1, n):
            s = lax.rem(me + d, n)
            remote(pieces.at[s, :, lane], parts.at[me, :, lane], rs_sem.at[0, group], rs_sem.at[1, group], "rows", s).start()

    def rs_sum(group):
        (lo, hi), lane = groups[group], group_lanes[group]
        arrived(parts.at[pl.ds(0, n - 1), :, lane], rs_sem.at[1, group])
        total = pieces[me, :, lane].astype(f32)
        for d in range(1, n):
            total = total + parts[lax.rem(me + n - d, n), :, lane].astype(f32)
        for slot in range(lo, hi):
            tile[slot] = total[:, (slot - lo) * own:(slot - lo + 1) * own].astype(bf16)

    def sym_slots(group):
        return range(max(1, groups[group][0]), groups[group][1])

    def sym_start(group):
        for slot in sym_slots(group):
            d = order[slot]
            there = rtile.at[order.index((zn - d) % zn)]
            remote(tile.at[slot], there, sy_sem.at[0, group], sy_sem.at[1, group], "feat", at_z(d)).start()

    def sym_bytes(group):
        return rtile.at[pl.ds(sym_slots(group)[0], len(sym_slots(group)))]

    def sym_end(group):
        if len(sym_slots(group)):
            arrived(sym_bytes(group), sy_sem.at[1, group])
        lo, hi = groups[group]
        for slot in range(lo, hi):
            both = tile[slot].astype(f32)
            if slot:
                both = both + rtile[slot].astype(f32)
            spiece[:, pl.ds(slot * own, own)] = both.astype(bf16)

    def gather_start(which, src, view):
        for d in range(1, h):
            there = lax.rem(chip + d, h)
            remote(src, view(chip, core), ag_sem.at[0, which], ag_sem.at[1, which], "rows", 2 * there + core).start()

    def gather_pass(which, view):
        arrived(view(pl.ds(0, h - 1), core), ag_sem.at[1, which])
        mine = view(pl.ds(0, h), core)
        copy = remote(mine, mine, am_sem.at[0, which], am_sem.at[1, which], "rows", mate)
        copy.start()
        return copy

    def s_view(group):
        return lambda chips, side: sall.at[chips, side, :, group_lanes[group]]

    def t_view(chips, side):
        return tall.at[chips, side]

    done = set()

    def take(arr, way, step, unit):
        if (arr, way, step, unit) not in done:
            done.add((arr, way, step, unit))
            hop(arr, way, step, unit).wait_recv()

    forwards = [(step, unit) for step in range(1, half) for unit in every]
    state = {"next": 0}

    def pump(count):
        for _ in range(count):
            if state["next"] < len(forwards):
                step, unit = forwards[state["next"]]
                state["next"] += 1
                for way in (0, 1):
                    if unit in units(step, way):
                        take(1, way, step - 1, unit)
                        hop(1, way, step, unit).start()

    def all_in(arr, dist):
        for unit in every:
            for way in (0, 1):
                if unit in units(dist - 1, way):
                    take(arr, way, dist - 1, unit)

    def center(rel):
        q = at_z(rel)
        xc_all[q] = (x_all[q].astype(f32) - means[q, 0:1]).astype(bf16)
    gram(0)
    product(0)
    v_second(0)
    rels = [[0]]
    for dist in range(1, half + 1):
        got = []
        for way in (0, 1):
            if way == 0 or dist < half:
                vhop(way, dist - 1).wait_recv()
                if (way == 0 and dist < half) or (way == 1 and dist < half - 1):
                    vhop(way, dist).start()
                rel = zn - dist if way == 0 else dist
                v_first(rel)
                got.append(rel)
        rels.append(got)
        for unit in every:
            for way in (0, 1):
                if unit in units(dist - 1, way):
                    take(0, way, dist - 1, unit)
                    if dist < half and unit in units(dist, way):
                        hop(0, way, dist, unit).start()
            if dist < half and unit == 1:
                for rel in rels[dist - 1]:
                    v_third(rel)
            if dist < half and unit == 2:
                for rel in rels[dist]:
                    v_second(rel)
        if dist == half - 1 or half == 1:
            for unit in every:
                for way in (0, 1):
                    if unit in units(0, way):
                        hop(1, way, 0, unit).start()
        if dist == 1:
            arrived(means.at[pl.ds(0, zn - 1)], me_sem.at[1])
        mine = [slot for slot in range(zn) if order[slot] in (dist, zn - dist)]
        if dist == 1 and split == 1:
            rs_start(0)
        for slot in mine:
            gram(slot)
            if dist < half:
                product(slot)
            if slot == split - 1:
                rs_start(0)
        if dist == half - 1:
            rs_sum(0)
            sym_start(0)
    rs_start(1)
    product(zn - 1)
    if half == 1:
        rs_sum(0)
        sym_start(0)
    sym_end(0)
    sall[chip, core, :, group_lanes[0]] = spiece[:, group_lanes[0]]
    gather_start(0, spiece.at[:, group_lanes[0]], s_view(0))
    if half > 1:
        for rel in rels[half - 1]:
            v_third(rel)
    else:
        v_third(0)
    pump(1)
    for rel in rels[half]:
        v_second(rel)
    rs_sum(1)
    sym_start(1)
    pump(2)
    passes = [gather_pass(0, s_view(0))]
    for rel in rels[half]:
        v_third(rel)
    pump(1)
    sym_end(1)
    sall[chip, core, :, group_lanes[1]] = spiece[:, group_lanes[1]]
    gather_start(1, spiece.at[:, group_lanes[1]], s_view(1))
    arrived(v_all.at[pl.ds(0, d_all // 2)], vd.at[1])
    vct[...] = v_all[:, lanes(chip, wide)].astype(f32).T.astype(bf16)
    yacc[...] = jnp.zeros_like(yacc)

    def y_part(group):
        passes[group].wait_recv()
        lo, hi = groups[group]
        for slot in range(lo, hi):
            q = at_z(order[slot])
            block = sall[:, :, :, pl.ds(slot * own, own)].astype(f32).reshape(own, own).astype(bf16)
            left = vct[rows_of(core, nar), lanes(q, own)]
            if slot == 0:
                yacc[...] += mm(left, block)
            else:
                @pl.when(q < z)
                def _():
                    yacc[...] += mm(left, block)

                @pl.when(q > z)
                def _():
                    yacc[...] += mm(left, block, 1, 1)

    y_part(0)
    pump(2)
    passes.append(gather_pass(1, s_view(1)))
    y_part(1)
    yown[...] = yacc[...].astype(bf16)
    for d in range(1, zn):
        remote(yown, yall.at[z], ya_sem.at[0], ya_sem.at[1], "feat", at_z(d)).start()
    yall[z] = yown[...]
    pump(2)
    if half > 1:
        all_in(1, 1)
        center(zn - 1)
        center(1)
    arrived(yall.at[pl.ds(0, zn - 1)], ya_sem.at[1])
    left = jnp.concatenate([yall[q] for q in range(zn)], axis=1)
    mt[...] = (kern[...] * mm(left, v_all[...])).astype(bf16)
    town[...] = mm(mt[...], v_all[rows_of(z, own)], 1, 1).astype(bf16)
    tall[chip, core] = town[...]
    gather_start(2, town, t_view)
    pump(len(forwards))
    if half > 2:
        all_in(1, 2)
        center(zn - 2)
        center(2)
    passes.append(gather_pass(2, t_view))
    passes[2].wait_recv()
    @pl.loop(0, zn)
    def _(q):
        part = mm(v_all[rows_of(q, own)], tall[...].reshape(d_all, own))
        sens[rows_of(q, own)] = ((2.0 / row_count) * part).astype(bf16)

    def finish(rel):
        q = at_z(rel)
        acc[...] += mm(xc_all[q], sens[rows_of(q, own)])
    finish(0)
    for dist in range(1, half):
        if dist > 2:
            all_in(1, dist)
            center(zn - dist)
            center(dist)
        finish(zn - dist)
        finish(dist)
    all_in(1, half)
    center(half)
    q = at_z(half)
    o_ref[...] = (acc[...] + mm(xc_all[q], sens[rows_of(q, own)])).astype(bf16)
    pair.wait_send()
    for arr, full in ((0, g_all), (1, x_all)):
        arrived(full.at[pl.ds(0, zn - 1)], ring_s.at[arr])
    v_arrived(zn - 1, vr_s.at[0])
    v_arrived(sum((ny if y_first(rel) else nx) - 1 for rel in range(zn)), v1_s.at[0])
    v_arrived(sum(ny * (nx - 1) if y_first(rel) else nx * (ny - 1) for rel in range(zn)), v2_s.at[0])
    arrived(v_all.at[pl.ds(0, d_all // 2)], vd.at[0])
    arrived(sums.at[pl.ds(0, n - 1)], su.at[0])
    arrived(means.at[pl.ds(0, zn - 1)], me_sem.at[0])
    for group in range(2):
        arrived(parts.at[pl.ds(0, n - 1), :, group_lanes[group]], rs_sem.at[0, group])
        if len(sym_slots(group)):
            arrived(sym_bytes(group), sy_sem.at[0, group])
        arrived(s_view(group)(pl.ds(0, h - 1), core), ag_sem.at[0, group])
    arrived(t_view(pl.ds(0, h - 1), core), ag_sem.at[0, 2])
    for copy in passes:
        copy.wait_send()
    arrived(yall.at[pl.ds(0, zn - 1)], ya_sem.at[0])


def local(features, grad_out, eigvecs, eigvals, whiten):
    tok, own = features.shape
    n, zn = lax.axis_size("rows"), lax.axis_size("feat")
    d_all = eigvals.shape[0]
    nar, rp = d_all // n, own // n
    h, half = n // 2, zn // 2
    row_count = tok * n
    scratch = [
        pltpu.VMEM((tok, own), bf16),
        pltpu.VMEM((tok, own), bf16),
        pltpu.VMEM((nar, own), f32),
        pltpu.VMEM((1, d_all), f32),
        pltpu.VMEM((d_all, own), bf16),
        pltpu.VMEM((zn, tok, own), bf16),
        pltpu.VMEM((zn, tok, own), bf16),
        pltpu.VMEM((zn, tok, own), bf16),
        pltpu.VMEM((d_all, d_all), bf16),
        pltpu.VMEM((2, nar, own), bf16),
        pltpu.VMEM((own, tok), bf16),
        pltpu.VMEM((tok, own), bf16),
        pltpu.VMEM((tok, own), f32),
        pltpu.VMEM((n, 8, own), f32),
        pltpu.VMEM((8, own), f32),
        pltpu.VMEM((zn, 8, own), f32),
        pltpu.VMEM((n, rp, d_all), bf16),
        pltpu.VMEM((n, rp, d_all), bf16),
        pltpu.VMEM((zn, rp, own), bf16),
        pltpu.VMEM((zn, rp, own), bf16),
        pltpu.VMEM((rp, d_all), bf16),
        pltpu.VMEM((h, 2, rp, d_all), bf16),
        pltpu.VMEM((2 * nar, d_all), bf16),
        pltpu.VMEM((nar, own), f32),
        pltpu.VMEM((nar, own), bf16),
        pltpu.VMEM((zn, nar, own), bf16),
        pltpu.VMEM((nar, d_all), f32),
        pltpu.VMEM((nar, d_all), bf16),
        pltpu.VMEM((nar, own), bf16),
        pltpu.VMEM((h, 2, nar, own), bf16),
        pltpu.VMEM((d_all, own), bf16),
    ]
    dma = pltpu.SemaphoreType.DMA
    scratch += [dma((5,)), dma((2,)), dma((2, 2, half, CHUNKS)), dma((1,)), dma((2, half)), dma((2,))]
    scratch += [dma((1,)), dma((zn,)), dma((1,)), dma((zn,)), dma((2,)), dma((2,)), dma((2,))]
    scratch += [dma((2, 2)), dma((2, 2)), dma((2, 3)), dma((2, 3)), dma((2,))]
    hbm = pl.BlockSpec(memory_space=pl.ANY)
    return pl.pallas_call(
        functools.partial(body, n, zn, row_count),
        out_shape=jax.ShapeDtypeStruct((tok, own), bf16),
        in_specs=[hbm] * 5,
        out_specs=VMEM,
        scratch_shapes=scratch,
        compiler_params=pltpu.CompilerParams(collective_id=1, has_side_effects=True, vmem_limit_bytes=58 * 2**20),
        cost_estimate=pl.CostEstimate(flops=8_000_000_000, bytes_accessed=16 * 2**20, transcendentals=0),
    )(features, grad_out, eigvecs.T, eigvals.reshape(1, d_all), whiten)


def solution(mesh):
    in_specs = (P("rows", "feat"), P("rows", "feat"), P("feat", "rows"), P(), P(None, "feat"))
    out_specs = P("rows", "feat")
    return jax.shard_map(local, mesh=mesh, in_specs=in_specs, out_specs=out_specs, check_vma=False)
```

```python
import functools
import math

import jax
import jax.numpy as jnp
from jax import lax
from jax.experimental import pallas as pl
from jax.experimental.pallas import tpu as pltpu
from jax.sharding import PartitionSpec as P

MESH = pl.DeviceIdType.MESH
VMEM = pl.BlockSpec(memory_space=pltpu.VMEM)
bf16, f32 = jnp.bfloat16, jnp.float32
CHUNKS = (4, 8)


def remote(src, dst, send, recv, axis, target):
    return pltpu.make_async_remote_copy(
        src_ref=src, dst_ref=dst, send_sem=send, recv_sem=recv,
        device_id={axis: target}, device_id_type=MESH,
    )


def lanes(index, width):
    return pl.ds(pl.multiple_of(index * width, width), width)


def mm(a, b, ca=1, cb=0):
    return lax.dot_general(a, b, (((ca,), (cb,)), ((), ())), preferred_element_type=f32)


def slot_order(zn):
    order = [0]
    for dist in range(1, zn // 2):
        order += [zn - dist, dist]
    return order + [zn // 2]


def body(n, zn, row_count, x_hbm, g_hbm, v_hbm, e_hbm, w_hbm, o_ref,
         x_ref, g_ref, v_ref, e_ref, w_ref, x_all, xc_all, g_all, v_all, v_col, v_pair, xct, gc, acc, sums, sums_own, means,
         pieces, parts, tile, rtile, spiece, sall, vct, yacc, yown, yall, kern, mt, town, tall, sens,
         ld, ring_s, ring_g, ring_x, vr_s, vr_r, vm, v1_s, v1_r, v2_s, v2_r, vd, vo, su, me_sem, rs_sem, sy_sem, ag_sem, am_sem, ya_sem):
    me, z = lax.axis_index("rows"), lax.axis_index("feat")
    core, chip = lax.rem(me, 2), me // 2
    mate = me + 1 - 2 * core
    h = n // 2
    nx = math.isqrt(h)
    ny = h // nx
    yy, xx = chip // nx, lax.rem(chip, nx)
    half = zn // 2
    tok, own = x_ref.shape
    d_all = v_all.shape[0]
    nar = d_all // n
    wide = 2 * nar
    hv = own // 2
    rp = own // n
    order = slot_order(zn)
    ring_r = (ring_g, ring_x)

    loads = []
    for i, (src, dst) in enumerate([(g_hbm, g_ref), (v_hbm, v_ref), (x_hbm, x_ref), (e_hbm, e_ref), (w_hbm, w_ref)]):
        load = pltpu.make_async_copy(src, dst, ld.at[i])
        load.start()
        loads.append(load)
    barrier = pltpu.get_barrier_semaphore()
    for d in range(1, n):
        pl.semaphore_signal(barrier, inc=1, device_id={"rows": lax.rem(me + d, n)}, device_id_type=MESH)
    for d in range(1, zn):
        pl.semaphore_signal(barrier, inc=1, device_id={"feat": lax.rem(z + d, zn)}, device_id_type=MESH)
    loads[0].wait()
    loads[1].wait()
    v_pair[core] = v_ref[...].astype(bf16)
    pl.semaphore_wait(barrier, n + zn - 2)

    def at_z(rel):
        return lax.rem(z + rel, zn)

    def rows_of(block, count):
        return pl.ds(pl.multiple_of(block * count, count), count)

    def arrived(ref, sem):
        pltpu.make_async_copy(ref, ref, sem).wait()

    def block_of(way, dist):
        return at_z(zn - dist) if way == 0 else at_z(dist)

    def next_of(way):
        return at_z(1) if way == 0 else at_z(zn - 1)

    def units(arr, step):
        return range(CHUNKS[arr] if step < half - 1 else CHUNKS[arr] // 2)

    def hop(arr, way, step, unit):
        full, mine = (g_all, g_ref) if arr == 0 else (x_all, x_ref)
        count = CHUNKS[arr]
        rows = pl.ds((unit + way * (count // 2)) % count * (tok // count), tok // count)
        there = full.at[block_of(way, step), rows]
        src = there if step else mine.at[rows]
        return remote(src, there, ring_s.at[arr], ring_r[arr].at[way, step, unit], "feat", next_of(way))

    def vpart(block, lane):
        return v_all.at[rows_of(2 * block + core, hv), lanes(lane, wide)]

    def v_mine(block):
        return v_col.at[rows_of(2 * block + core, hv)]

    def v_keep(block):
        rows = rows_of(2 * block + core, hv)
        v_all[rows, lanes(chip, wide)] = v_col[rows]

    def v_arrived(count, sem):
        if count * wide > d_all:
            arrived(v_all.at[pl.ds(0, count * wide * hv // d_all)], sem)
        elif count:
            arrived(v_all.at[pl.ds(0, hv), pl.ds(0, count * wide)], sem)

    def vhop(way, step):
        ref = v_mine(block_of(way, step))
        return remote(ref, ref, vr_s.at[0], vr_r.at[way, step], "feat", next_of(way))

    def y_first(rel):
        return rel == 0 or rel > half

    def by_y(d):
        return (lax.rem(yy + d, ny) * nx + xx) * 2 + core

    def by_x(d):
        return (yy * nx + lax.rem(xx + d, nx)) * 2 + core

    def v_first(rel):
        src, ref = v_mine(at_z(rel)), vpart(at_z(rel), chip)
        if rel:
            remote(src, src, vo.at[0], vo.at[1], "rows", mate).start()
        v_keep(at_z(rel))
        for d in range(1, ny if y_first(rel) else nx):
            target = by_y(d) if y_first(rel) else by_x(d)
            remote(src, ref, v1_s.at[0], v1_r.at[rel], "rows", target).start()

    def v_second(rel):
        v_arrived((ny if y_first(rel) else nx) - 1, v1_r.at[rel])
        if y_first(rel):
            for e in range(ny):
                ref = vpart(at_z(rel), lax.rem(yy + ny - e, ny) * nx + xx)
                src = ref if e else v_mine(at_z(rel))
                for d in range(1, nx):
                    remote(src, ref, v2_s.at[0], v2_r.at[rel], "rows", by_x(d)).start()
        else:
            ref = v_all.at[rows_of(2 * at_z(rel) + core, hv), lanes(yy, nx * wide)]
            for d in range(1, ny):
                remote(ref, ref, v2_s.at[0], v2_r.at[rel], "rows", by_y(d)).start()

    def v_third(rel):
        v_arrived(ny * (nx - 1) if y_first(rel) else nx * (ny - 1), v2_r.at[rel])
        ref = v_all.at[rows_of(2 * at_z(rel) + core, hv)]
        remote(ref, ref, vd.at[0], vd.at[1], "rows", mate).start()

    for way in (0, 1):
        hop(0, way, 0, 0).start()
    pair = remote(v_pair.at[core], v_pair.at[core], vm.at[0], vm.at[1], "rows", mate)
    pair.start()
    loads[2].wait()
    sums_own[...] = jnp.zeros_like(sums_own)
    sums_own[0:1] = jnp.sum(x_ref[...].astype(f32), axis=0, keepdims=True)
    sums_own[1:2] = jnp.sum(g_ref[...].astype(f32), axis=0, keepdims=True)
    pair.wait_recv()
    both = jnp.concatenate([v_pair[0].astype(f32), v_pair[1].astype(f32)], axis=0)
    v_col[rows_of(z, own)] = both.T.astype(bf16)
    for way in (0, 1):
        if way == 0 or half > 1:
            vhop(way, 0).start()
        for unit in units(0, 0)[1:]:
            hop(0, way, 0, unit).start()
    for d in range(1, n):
        remote(sums_own, sums.at[me], su.at[0], su.at[1], "rows", lax.rem(me + d, n)).start()
    sums[me] = sums_own[...]
    v_first(0)

    loads[3].wait()
    root = jnp.sqrt(e_ref[...])
    shape = (nar, d_all)
    wanted = me * nar + lax.broadcasted_iota(jnp.int32, shape, 0)
    hit = wanted == lax.broadcasted_iota(jnp.int32, shape, 1)
    root_row = jnp.sum(jnp.where(hit, jnp.broadcast_to(root, shape), 0.0), axis=1, keepdims=True)
    kern[...] = -1.0 / ((root_row * root) * (root_row + root))

    arrived(sums.at[pl.ds(0, n - 1)], su.at[1])
    means[z] = jnp.sum(sums[...], axis=0) / row_count
    for d in range(1, zn):
        remote(means.at[z], means.at[z], me_sem.at[0], me_sem.at[1], "feat", at_z(d)).start()
    xc = x_ref[...].astype(f32) - means[z, 0:1]
    xc_all[z] = xc.astype(bf16)
    xct[...] = xc.T.astype(bf16)
    loads[4].wait()

    def gram(slot):
        rel = order[slot]
        q = at_z(rel)
        src = g_ref if rel == 0 else g_all.at[q]
        gc[...] = (src[...].astype(f32) - means[q, 1:2]).astype(bf16)
        block = mm(xct[...], gc[...])
        lane = pl.ds(slot * own, own)

        def put(value):
            pieces[:, :, lane] = value.reshape(n, rp, own).astype(bf16)

        if rel == 0:
            put(0.5 * (block + block.T))
        else:
            @pl.when(z < q)
            def _():
                put(0.5 * block)

            @pl.when(z > q)
            def _():
                put(0.5 * block.T)

    def product(slot):
        gw = mm(gc[...], w_ref[rows_of(at_z(order[slot]), own)])
        acc[...] = gw if slot == 0 else acc[...] + gw

    split = max(1, zn - 3)
    groups = [(lo, hi) for lo, hi in ((0, split), (split, zn - 1), (zn - 1, zn)) if lo < hi]
    last = len(groups) - 1
    group_lanes = [pl.ds(lo * own, (hi - lo) * own) for lo, hi in groups]

    def rs_start(group):
        lane = group_lanes[group]
        for d in range(1, n):
            s = lax.rem(me + d, n)
            remote(pieces.at[s, :, lane], parts.at[me, :, lane], rs_sem.at[0, group], rs_sem.at[1, group], "rows", s).start()

    def rs_sum(group):
        (lo, hi), lane = groups[group], group_lanes[group]
        arrived(parts.at[pl.ds(0, n - 1), :, lane], rs_sem.at[1, group])
        total = pieces[me, :, lane].astype(f32)
        for d in range(1, n):
            total = total + parts[lax.rem(me + n - d, n), :, lane].astype(f32)
        for slot in range(lo, hi):
            tile[slot] = total[:, (slot - lo) * own:(slot - lo + 1) * own].astype(bf16)

    def sym_slots(group):
        return range(max(1, groups[group][0]), groups[group][1])

    def sym_start(group):
        for slot in sym_slots(group):
            d = order[slot]
            there = rtile.at[order.index((zn - d) % zn)]
            remote(tile.at[slot], there, sy_sem.at[0, group], sy_sem.at[1, group], "feat", at_z(d)).start()

    def sym_bytes(group):
        return rtile.at[pl.ds(sym_slots(group)[0], len(sym_slots(group)))]

    def sym_end(group):
        if len(sym_slots(group)):
            arrived(sym_bytes(group), sy_sem.at[1, group])
        lo, hi = groups[group]
        for slot in range(lo, hi):
            both = tile[slot].astype(f32)
            if slot:
                both = both + rtile[slot].astype(f32)
            spiece[:, pl.ds(slot * own, own)] = both.astype(bf16)

    def gather_start(which, src, view):
        for d in range(1, h):
            there = lax.rem(chip + d, h)
            remote(src, view(chip, core), ag_sem.at[0, which], ag_sem.at[1, which], "rows", 2 * there + core).start()

    def gather_pass(which, view):
        arrived(view(pl.ds(0, h - 1), core), ag_sem.at[1, which])
        mine = view(pl.ds(0, h), core)
        copy = remote(mine, mine, am_sem.at[0, which], am_sem.at[1, which], "rows", mate)
        copy.start()
        return copy

    def s_view(group):
        return lambda chips, side: sall.at[chips, side, :, group_lanes[group]]

    def t_view(chips, side):
        return tall.at[chips, side]

    done = set()

    def take(arr, way, step, unit):
        if (arr, way, step, unit) not in done:
            done.add((arr, way, step, unit))
            hop(arr, way, step, unit).wait_recv()

    forwards = [(step, unit) for step in range(half) for unit in units(1, step)]
    state = {"next": 0}

    def pump(count):
        for _ in range(count):
            if state["next"] < len(forwards):
                step, unit = forwards[state["next"]]
                state["next"] += 1
                for way in (0, 1):
                    if step:
                        take(1, way, step - 1, unit)
                    hop(1, way, step, unit).start()

    def all_in(arr, dist):
        for unit in units(arr, dist - 1):
            for way in (0, 1):
                take(arr, way, dist - 1, unit)

    def center(rel):
        q = at_z(rel)
        xc_all[q] = (x_all[q].astype(f32) - means[q, 0:1]).astype(bf16)

    gram(0)
    if split == 1:
        rs_start(0)
    product(0)
    v_second(0)
    rels = [[0]]
    for dist in range(1, half + 1):
        got = []
        for way in (0, 1):
            if way == 0 or dist < half:
                vhop(way, dist - 1).wait_recv()
                if (way == 0 and dist < half) or (way == 1 and dist < half - 1):
                    vhop(way, dist).start()
                rel = zn - dist if way == 0 else dist
                v_first(rel)
                got.append(rel)
        rels.append(got)
        for unit in units(0, dist - 1):
            for way in (0, 1):
                take(0, way, dist - 1, unit)
                if dist < half and unit in units(0, dist):
                    hop(0, way, dist, unit).start()
            if dist == half - 1 and unit >= CHUNKS[0] // 2:
                pump(2)
            if dist == half:
                pump(2 - unit)
            if dist >= 2 and unit == 1:
                for rel in rels[dist - 2]:
                    v_third(rel)
        if dist == 1:
            arrived(means.at[pl.ds(0, zn - 1)], me_sem.at[1])
        mine = [slot for slot in range(zn) if order[slot] in (dist, zn - dist)]
        for slot in mine:
            gram(slot)
            for group in range(last):
                if slot == groups[group][1] - 1:
                    rs_start(group)
            if dist < half:
                product(slot)
        if dist == half - 1:
            rs_sum(0)
            sym_start(0)
        if dist < half - 1:
            for rel in rels[dist]:
                v_second(rel)
    rs_start(last)
    product(zn - 1)
    for group in range(1 if half > 1 else 0, last):
        rs_sum(group)
        sym_start(group)
    pump(1)
    if half > 1:
        for rel in rels[half - 1]:
            v_second(rel)
    pump(2)
    rs_sum(last)
    sym_start(last)
    pump(2)

    def s_start(group):
        sym_end(group)
        lane = group_lanes[group]
        sall[chip, core, :, lane] = spiece[:, lane]
        gather_start(group, spiece.at[:, lane], s_view(group))

    for group in range(last):
        s_start(group)
    for rel in rels[half]:
        v_second(rel)
    pump(2)
    s_start(last)
    pump(1)
    passes = [gather_pass(group, s_view(group)) for group in range(last)]
    v_arrived(zn - 1, vo.at[1])
    vct[...] = v_col[...].astype(f32).T.astype(bf16)
    yacc[...] = jnp.zeros_like(yacc)

    def y_part(group):
        passes[group].wait_recv()
        lo, hi = groups[group]
        for slot in range(lo, hi):
            q = at_z(order[slot])
            block = sall[:, :, :, pl.ds(slot * own, own)].astype(f32).reshape(own, own).astype(bf16)
            left = vct[rows_of(core, nar), lanes(q, own)]
            if slot == 0:
                yacc[...] += mm(left, block)
            else:
                @pl.when(q < z)
                def _():
                    yacc[...] += mm(left, block)

                @pl.when(q > z)
                def _():
                    yacc[...] += mm(left, block, 1, 1)

    for group in range(last):
        y_part(group)
    pump(2)
    passes.append(gather_pass(last, s_view(last)))
    y_part(last)
    yown[...] = yacc[...].astype(bf16)
    for d in range(1, zn):
        remote(yown, yall.at[z], ya_sem.at[0], ya_sem.at[1], "feat", at_z(d)).start()
    yall[z] = yown[...]
    for rel in rels[half - 1] + rels[half]:
        v_third(rel)
    pump(1)
    if half > 1:
        all_in(1, 1)
        center(zn - 1)
        center(1)
    arrived(yall.at[pl.ds(0, zn - 1)], ya_sem.at[1])
    arrived(v_all.at[pl.ds(0, d_all // 2)], vd.at[1])
    left = jnp.concatenate([yall[q] for q in range(zn)], axis=1)
    mt[...] = (kern[...] * mm(left, v_all[...])).astype(bf16)
    town[...] = mm(mt[...], v_all[rows_of(z, own)], 1, 1).astype(bf16)
    tall[chip, core] = town[...]
    gather_start(3, town, t_view)
    pump(6)
    if half > 2:
        all_in(1, 2)
        center(zn - 2)
        center(2)
    passes.append(gather_pass(3, t_view))
    pump(2)
    passes[-1].wait_recv()
    pump(len(forwards))

    step_rows = d_all // 4

    @pl.loop(0, 4)
    def _(q):
        part = mm(v_all[rows_of(q, step_rows)], tall[...].reshape(d_all, own))
        sens[rows_of(q, step_rows)] = ((2.0 / row_count) * part).astype(bf16)

    def finish(rel):
        q = at_z(rel)
        acc[...] += mm(xc_all[q], sens[rows_of(q, own)])

    finish(0)
    for dist in range(1, half):
        if dist > 2:
            all_in(1, dist)
            center(zn - dist)
            center(dist)
        finish(zn - dist)
        finish(dist)
    all_in(1, half)
    center(half)
    q = at_z(half)
    o_ref[...] = (acc[...] + mm(xc_all[q], sens[rows_of(q, own)])).astype(bf16)

    pair.wait_send()
    for arr, full in ((0, g_all), (1, x_all)):
        arrived(full.at[pl.ds(0, zn - 1)], ring_s.at[arr])
    v_arrived(zn - 1, vr_s.at[0])
    v_arrived(sum((ny if y_first(rel) else nx) - 1 for rel in range(zn)), v1_s.at[0])
    v_arrived(sum(ny * (nx - 1) if y_first(rel) else nx * (ny - 1) for rel in range(zn)), v2_s.at[0])
    arrived(v_all.at[pl.ds(0, d_all // 2)], vd.at[0])
    v_arrived(zn - 1, vo.at[0])
    arrived(sums.at[pl.ds(0, n - 1)], su.at[0])
    arrived(means.at[pl.ds(0, zn - 1)], me_sem.at[0])
    for group in range(last + 1):
        arrived(parts.at[pl.ds(0, n - 1), :, group_lanes[group]], rs_sem.at[0, group])
        if len(sym_slots(group)):
            arrived(sym_bytes(group), sy_sem.at[0, group])
        arrived(s_view(group)(pl.ds(0, h - 1), core), ag_sem.at[0, group])
    arrived(t_view(pl.ds(0, h - 1), core), ag_sem.at[0, 3])
    for copy in passes:
        copy.wait_send()
    arrived(yall.at[pl.ds(0, zn - 1)], ya_sem.at[0])


def local(features, grad_out, eigvecs, eigvals, whiten):
    tok, own = features.shape
    n, zn = lax.axis_size("rows"), lax.axis_size("feat")
    d_all = eigvals.shape[0]
    nar, rp = d_all // n, own // n
    h, half = n // 2, zn // 2
    row_count = tok * n
    scratch = [
        pltpu.VMEM((tok, own), bf16),
        pltpu.VMEM((tok, own), bf16),
        pltpu.VMEM((nar, own), f32),
        pltpu.VMEM((1, d_all), f32),
        pltpu.VMEM((d_all, own), bf16),
        pltpu.VMEM((zn, tok, own), bf16),
        pltpu.VMEM((zn, tok, own), bf16),
        pltpu.VMEM((zn, tok, own), bf16),
        pltpu.VMEM((d_all, d_all), bf16),
        pltpu.VMEM((d_all, 2 * nar), bf16),
        pltpu.VMEM((2, nar, own), bf16),
        pltpu.VMEM((own, tok), bf16),
        pltpu.VMEM((tok, own), bf16),
        pltpu.VMEM((tok, own), f32),
        pltpu.VMEM((n, 8, own), f32),
        pltpu.VMEM((8, own), f32),
        pltpu.VMEM((zn, 8, own), f32),
        pltpu.VMEM((n, rp, d_all), bf16),
        pltpu.VMEM((n, rp, d_all), bf16),
        pltpu.VMEM((zn, rp, own), bf16),
        pltpu.VMEM((zn, rp, own), bf16),
        pltpu.VMEM((rp, d_all), bf16),
        pltpu.VMEM((h, 2, rp, d_all), bf16),
        pltpu.VMEM((2 * nar, d_all), bf16),
        pltpu.VMEM((nar, own), f32),
        pltpu.VMEM((nar, own), bf16),
        pltpu.VMEM((zn, nar, own), bf16),
        pltpu.VMEM((nar, d_all), f32),
        pltpu.VMEM((nar, d_all), bf16),
        pltpu.VMEM((nar, own), bf16),
        pltpu.VMEM((h, 2, nar, own), bf16),
        pltpu.VMEM((d_all, own), bf16),
    ]
    dma = pltpu.SemaphoreType.DMA
    scratch += [dma((5,)), dma((2,)), dma((2, half, CHUNKS[0])), dma((2, half, CHUNKS[1])), dma((1,)), dma((2, half)), dma((2,))]
    scratch += [dma((1,)), dma((zn,)), dma((1,)), dma((zn,)), dma((2,)), dma((2,)), dma((2,)), dma((2,))]
    scratch += [dma((2, 3)), dma((2, 3)), dma((2, 4)), dma((2, 4)), dma((2,))]
    hbm = pl.BlockSpec(memory_space=pl.ANY)
    return pl.pallas_call(
        functools.partial(body, n, zn, row_count),
        out_shape=jax.ShapeDtypeStruct((tok, own), bf16),
        in_specs=[hbm] * 5,
        out_specs=VMEM,
        scratch_shapes=scratch,
        compiler_params=pltpu.CompilerParams(collective_id=1, has_side_effects=True, vmem_limit_bytes=58 * 2**20),
        cost_estimate=pl.CostEstimate(flops=8_000_000_000, bytes_accessed=16 * 2**20, transcendentals=0),
    )(features, grad_out, eigvecs.T, eigvals.reshape(1, d_all), whiten)


def solution(mesh):
    in_specs = (P("rows", "feat"), P("rows", "feat"), P("feat", "rows"), P(), P(None, "feat"))
    out_specs = P("rows", "feat")
    return jax.shard_map(local, mesh=mesh, in_specs=in_specs, out_specs=out_specs, check_vma=False)
```

```python
import functools
import math

import jax
import jax.numpy as jnp
from jax import lax
from jax.experimental import pallas as pl
from jax.experimental.pallas import tpu as pltpu
from jax.sharding import PartitionSpec as P

MESH = pl.DeviceIdType.MESH
VMEM = pl.BlockSpec(memory_space=pltpu.VMEM)
bf16, f32 = jnp.bfloat16, jnp.float32
CHUNKS = (4, 8)


def remote(src, dst, send, recv, axis, target):
    return pltpu.make_async_remote_copy(
        src_ref=src, dst_ref=dst, send_sem=send, recv_sem=recv,
        device_id={axis: target}, device_id_type=MESH,
    )


def lanes(index, width):
    return pl.ds(pl.multiple_of(index * width, width), width)


def mm(a, b, ca=1, cb=0):
    return lax.dot_general(a, b, (((ca,), (cb,)), ((), ())), preferred_element_type=f32)


def slot_order(zn):
    order = [0]
    for dist in range(1, zn // 2):
        order += [zn - dist, dist]
    return order + [zn // 2]


def body(n, zn, row_count, x_hbm, g_hbm, v_hbm, e_hbm, w_hbm, o_ref,
         x_ref, g_ref, v_ref, e_ref, w_ref, x_all, xc_all, g_all, v_all, v_col, v_pair, xct, gc, acc, sums, sums_own, means,
         pieces, parts, tile, rtile, spiece, sall, vct, yacc, yown, yall, kern, mt, town, tall, sens,
         ld, ring_s, ring_g, ring_x, vr_s, vr_r, vm, v1_s, v1_r, v2_s, v2_r, vd, vo, su, me_sem, rs_sem, sy_sem, ag_sem, am_sem, ya_sem):
    me, z = lax.axis_index("rows"), lax.axis_index("feat")
    core, chip = lax.rem(me, 2), me // 2
    mate = me + 1 - 2 * core
    h = n // 2
    nx = math.isqrt(h)
    ny = h // nx
    yy, xx = chip // nx, lax.rem(chip, nx)
    half = zn // 2
    tok, own = x_ref.shape
    d_all = v_all.shape[0]
    nar = d_all // n
    wide = 2 * nar
    hv = own // 2
    rp = own // n
    order = slot_order(zn)
    ring_r = (ring_g, ring_x)

    loads = []
    for i, (src, dst) in enumerate([(g_hbm, g_ref), (v_hbm, v_ref), (x_hbm, x_ref), (e_hbm, e_ref), (w_hbm, w_ref)]):
        load = pltpu.make_async_copy(src, dst, ld.at[i])
        load.start()
        loads.append(load)
    barrier = pltpu.get_barrier_semaphore()
    for d in range(1, n):
        pl.semaphore_signal(barrier, inc=1, device_id={"rows": lax.rem(me + d, n)}, device_id_type=MESH)
    for d in range(1, zn):
        pl.semaphore_signal(barrier, inc=1, device_id={"feat": lax.rem(z + d, zn)}, device_id_type=MESH)
    loads[0].wait()
    loads[1].wait()
    v_pair[core] = v_ref[...].astype(bf16)
    pl.semaphore_wait(barrier, n + zn - 2)

    def at_z(rel):
        return lax.rem(z + rel, zn)

    def rows_of(block, count):
        return pl.ds(pl.multiple_of(block * count, count), count)

    def arrived(ref, sem):
        pltpu.make_async_copy(ref, ref, sem).wait()

    def block_of(way, dist):
        return at_z(zn - dist) if way == 0 else at_z(dist)

    def next_of(way):
        return at_z(1) if way == 0 else at_z(zn - 1)

    def units(arr, step):
        return range(CHUNKS[arr] if step < half - 1 else CHUNKS[arr] // 2)

    def hop(arr, way, step, unit):
        full, mine = (g_all, g_ref) if arr == 0 else (x_all, x_ref)
        count = CHUNKS[arr]
        rows = pl.ds((unit + way * (count // 2)) % count * (tok // count), tok // count)
        there = full.at[block_of(way, step), rows]
        src = there if step else mine.at[rows]
        return remote(src, there, ring_s.at[arr], ring_r[arr].at[way, step, unit], "feat", next_of(way))

    def vpart(block, lane):
        return v_all.at[rows_of(2 * block + core, hv), lanes(lane, wide)]

    def v_mine(block):
        return v_col.at[rows_of(2 * block + core, hv)]

    def v_keep(block):
        rows = rows_of(2 * block + core, hv)
        v_all[rows, lanes(chip, wide)] = v_col[rows]

    def v_arrived(count, sem):
        if count * wide > d_all:
            arrived(v_all.at[pl.ds(0, count * wide * hv // d_all)], sem)
        elif count:
            arrived(v_all.at[pl.ds(0, hv), pl.ds(0, count * wide)], sem)

    def vhop(way, step):
        ref = v_mine(block_of(way, step))
        return remote(ref, ref, vr_s.at[0], vr_r.at[way, step], "feat", next_of(way))

    def y_first(rel):
        return rel == 0 or rel > half

    def by_y(d):
        return (lax.rem(yy + d, ny) * nx + xx) * 2 + core

    def by_x(d):
        return (yy * nx + lax.rem(xx + d, nx)) * 2 + core

    def v_first(rel):
        src, ref = v_mine(at_z(rel)), vpart(at_z(rel), chip)
        if rel:
            remote(src, src, vo.at[0], vo.at[1], "rows", mate).start()
        v_keep(at_z(rel))
        for d in range(1, ny if y_first(rel) else nx):
            target = by_y(d) if y_first(rel) else by_x(d)
            remote(src, ref, v1_s.at[0], v1_r.at[rel], "rows", target).start()

    def v_second(rel):
        v_arrived((ny if y_first(rel) else nx) - 1, v1_r.at[rel])
        if y_first(rel):
            for e in range(ny):
                ref = vpart(at_z(rel), lax.rem(yy + ny - e, ny) * nx + xx)
                src = ref if e else v_mine(at_z(rel))
                for d in range(1, nx):
                    remote(src, ref, v2_s.at[0], v2_r.at[rel], "rows", by_x(d)).start()
        else:
            ref = v_all.at[rows_of(2 * at_z(rel) + core, hv), lanes(yy, nx * wide)]
            for d in range(1, ny):
                remote(ref, ref, v2_s.at[0], v2_r.at[rel], "rows", by_y(d)).start()

    def v_third(rel):
        v_arrived(ny * (nx - 1) if y_first(rel) else nx * (ny - 1), v2_r.at[rel])
        ref = v_all.at[rows_of(2 * at_z(rel) + core, hv)]
        remote(ref, ref, vd.at[0], vd.at[1], "rows", mate).start()

    for way in (0, 1):
        hop(0, way, 0, 0).start()
    pair = remote(v_pair.at[core], v_pair.at[core], vm.at[0], vm.at[1], "rows", mate)
    pair.start()
    loads[2].wait()
    sums_own[...] = jnp.zeros_like(sums_own)
    sums_own[0:1] = jnp.sum(x_ref[...].astype(f32), axis=0, keepdims=True)
    sums_own[1:2] = jnp.sum(g_ref[...].astype(f32), axis=0, keepdims=True)
    pair.wait_recv()
    both = jnp.concatenate([v_pair[0].astype(f32), v_pair[1].astype(f32)], axis=0)
    v_col[rows_of(z, own)] = both.T.astype(bf16)
    for way in (0, 1):
        if way == 0 or half > 1:
            vhop(way, 0).start()
        for unit in units(0, 0)[1:]:
            hop(0, way, 0, unit).start()
    for d in range(1, n):
        remote(sums_own, sums.at[me], su.at[0], su.at[1], "rows", lax.rem(me + d, n)).start()
    sums[me] = sums_own[...]
    v_first(0)

    loads[3].wait()
    root = jnp.sqrt(e_ref[...])
    shape = (nar, d_all)
    wanted = me * nar + lax.broadcasted_iota(jnp.int32, shape, 0)
    hit = wanted == lax.broadcasted_iota(jnp.int32, shape, 1)
    root_row = jnp.sum(jnp.where(hit, jnp.broadcast_to(root, shape), 0.0), axis=1, keepdims=True)
    kern[...] = -1.0 / ((root_row * root) * (root_row + root))

    arrived(sums.at[pl.ds(0, n - 1)], su.at[1])
    means[z] = jnp.sum(sums[...], axis=0) / row_count
    for d in range(1, zn):
        remote(means.at[z], means.at[z], me_sem.at[0], me_sem.at[1], "feat", at_z(d)).start()
    xc = x_ref[...].astype(f32) - means[z, 0:1]
    xc_all[z] = xc.astype(bf16)
    xct[...] = xc.T.astype(bf16)
    loads[4].wait()

    def gram(slot):
        rel = order[slot]
        q = at_z(rel)
        src = g_ref if rel == 0 else g_all.at[q]
        gc[...] = (src[...].astype(f32) - means[q, 1:2]).astype(bf16)
        block = mm(xct[...], gc[...])
        lane = pl.ds(slot * own, own)

        def put(value):
            pieces[:, :, lane] = value.reshape(n, rp, own).astype(bf16)

        if rel == 0:
            put(0.5 * (block + block.T))
        else:
            @pl.when(z < q)
            def _():
                put(0.5 * block)

            @pl.when(z > q)
            def _():
                put(0.5 * block.T)

    def product(slot):
        gw = mm(gc[...], w_ref[rows_of(at_z(order[slot]), own)])
        acc[...] = gw if slot == 0 else acc[...] + gw

    split = max(1, zn - 3)
    groups = [(lo, hi) for lo, hi in ((0, split), (split, zn - 1), (zn - 1, zn)) if lo < hi]
    last = len(groups) - 1
    group_lanes = [pl.ds(lo * own, (hi - lo) * own) for lo, hi in groups]

    def rs_start(group):
        lane = group_lanes[group]
        for d in range(1, n):
            s = lax.rem(me + d, n)
            remote(pieces.at[s, :, lane], parts.at[me, :, lane], rs_sem.at[0, group], rs_sem.at[1, group], "rows", s).start()

    def rs_sum(group):
        (lo, hi), lane = groups[group], group_lanes[group]
        arrived(parts.at[pl.ds(0, n - 1), :, lane], rs_sem.at[1, group])
        total = pieces[me, :, lane].astype(f32)
        for d in range(1, n):
            total = total + parts[lax.rem(me + n - d, n), :, lane].astype(f32)
        for slot in range(lo, hi):
            tile[slot] = total[:, (slot - lo) * own:(slot - lo + 1) * own].astype(bf16)

    def sym_slots(group):
        return range(max(1, groups[group][0]), groups[group][1])

    def sym_start(group):
        for slot in sym_slots(group):
            d = order[slot]
            there = rtile.at[order.index((zn - d) % zn)]
            remote(tile.at[slot], there, sy_sem.at[0, group], sy_sem.at[1, group], "feat", at_z(d)).start()

    def sym_bytes(group):
        return rtile.at[pl.ds(sym_slots(group)[0], len(sym_slots(group)))]

    def sym_end(group):
        if len(sym_slots(group)):
            arrived(sym_bytes(group), sy_sem.at[1, group])
        lo, hi = groups[group]
        for slot in range(lo, hi):
            both = tile[slot].astype(f32)
            if slot:
                both = both + rtile[slot].astype(f32)
            spiece[:, pl.ds(slot * own, own)] = both.astype(bf16)

    def gather_start(which, src, view):
        for d in range(1, h):
            there = lax.rem(chip + d, h)
            remote(src, view(chip, core), ag_sem.at[0, which], ag_sem.at[1, which], "rows", 2 * there + core).start()

    def gather_pass(which, view):
        arrived(view(pl.ds(0, h - 1), core), ag_sem.at[1, which])
        mine = view(pl.ds(0, h), core)
        copy = remote(mine, mine, am_sem.at[0, which], am_sem.at[1, which], "rows", mate)
        copy.start()
        return copy

    def s_view(group):
        return lambda chips, side: sall.at[chips, side, :, group_lanes[group]]

    def t_view(chips, side):
        return tall.at[chips, side]

    done = set()

    def take(arr, way, step, unit):
        if (arr, way, step, unit) not in done:
            done.add((arr, way, step, unit))
            hop(arr, way, step, unit).wait_recv()

    forwards = [(step, unit) for step in range(half) for unit in units(1, step)]
    state = {"next": 0}

    def pump(count):
        for _ in range(count):
            if state["next"] < len(forwards):
                step, unit = forwards[state["next"]]
                state["next"] += 1
                for way in (0, 1):
                    if step:
                        take(1, way, step - 1, unit)
                    hop(1, way, step, unit).start()

    def all_in(arr, dist):
        for unit in units(arr, dist - 1):
            for way in (0, 1):
                take(arr, way, dist - 1, unit)

    def center(rel):
        q = at_z(rel)
        xc_all[q] = (x_all[q].astype(f32) - means[q, 0:1]).astype(bf16)

    gram(0)
    if split == 1:
        rs_start(0)
    product(0)
    v_second(0)
    rels = [[0]]
    for dist in range(1, half + 1):
        got = []
        for way in (0, 1):
            if way == 0 or dist < half:
                vhop(way, dist - 1).wait_recv()
                if (way == 0 and dist < half) or (way == 1 and dist < half - 1):
                    vhop(way, dist).start()
                rel = zn - dist if way == 0 else dist
                v_first(rel)
                got.append(rel)
        rels.append(got)
        for unit in units(0, dist - 1):
            for way in (0, 1):
                take(0, way, dist - 1, unit)
                if dist < half and unit in units(0, dist):
                    hop(0, way, dist, unit).start()
            if dist == half - 1 and unit == 1:
                rs_sum(0)
                sym_start(0)
            if dist == half - 1 and unit == 3:
                pump(2)
            if dist == half:
                pump(1)
            if dist >= 2 and unit == 1:
                for rel in rels[dist - 2]:
                    v_third(rel)
        if dist == 1:
            arrived(means.at[pl.ds(0, zn - 1)], me_sem.at[1])
        mine = [slot for slot in range(zn) if order[slot] in (dist, zn - dist)]
        for slot in mine:
            gram(slot)
            for group in range(last):
                if slot == groups[group][1] - 1:
                    rs_start(group)
            if dist < half:
                product(slot)
        if dist < half - 1:
            for rel in rels[dist]:
                v_second(rel)
    def s_start(group):
        sym_end(group)
        lane = group_lanes[group]
        sall[chip, core, :, lane] = spiece[:, lane]
        gather_start(group, spiece.at[:, lane], s_view(group))

    rs_start(last)
    product(zn - 1)
    if half == 1:
        rs_sum(0)
        sym_start(0)
    s_start(0)
    if half > 1:
        for rel in rels[half - 1]:
            v_second(rel)
    for group in range(1, last):
        rs_sum(group)
        sym_start(group)
    pump(2)
    rs_sum(last)
    sym_start(last)
    pump(2)
    for group in range(1, last):
        s_start(group)
    pump(2)
    s_start(last)
    for rel in rels[half]:
        v_second(rel)
    pump(4)
    passes = [gather_pass(group, s_view(group)) for group in range(last)]
    v_arrived(zn - 1, vo.at[1])
    vct[...] = v_col[...].astype(f32).T.astype(bf16)
    yacc[...] = jnp.zeros_like(yacc)

    def y_part(group):
        passes[group].wait_recv()
        lo, hi = groups[group]
        for slot in range(lo, hi):
            q = at_z(order[slot])
            block = sall[:, :, :, pl.ds(slot * own, own)].astype(f32).reshape(own, own).astype(bf16)
            left = vct[rows_of(core, nar), lanes(q, own)]
            if slot == 0:
                yacc[...] += mm(left, block)
            else:
                @pl.when(q < z)
                def _():
                    yacc[...] += mm(left, block)

                @pl.when(q > z)
                def _():
                    yacc[...] += mm(left, block, 1, 1)

    for group in range(last):
        y_part(group)
    pump(1)
    passes.append(gather_pass(last, s_view(last)))
    y_part(last)
    yown[...] = yacc[...].astype(bf16)
    for d in range(1, zn):
        remote(yown, yall.at[z], ya_sem.at[0], ya_sem.at[1], "feat", at_z(d)).start()
    yall[z] = yown[...]
    for rel in rels[half - 1] + rels[half]:
        v_third(rel)
    pump(2)
    if half > 1:
        all_in(1, 1)
        center(zn - 1)
        center(1)
    arrived(yall.at[pl.ds(0, zn - 1)], ya_sem.at[1])
    pump(4)
    arrived(v_all.at[pl.ds(0, d_all // 2)], vd.at[1])
    left = jnp.concatenate([yall[q] for q in range(zn)], axis=1)
    mt[...] = (kern[...] * mm(left, v_all[...])).astype(bf16)
    town[...] = mm(mt[...], v_all[rows_of(z, own)], 1, 1).astype(bf16)
    tall[chip, core] = town[...]
    gather_start(3, town, t_view)
    pump(4)
    if half > 2:
        all_in(1, 2)
        center(zn - 2)
        center(2)
    pump(2)
    passes.append(gather_pass(3, t_view))
    pump(len(forwards))
    passes[-1].wait_recv()
    step_rows = d_all // 4

    @pl.loop(0, 4)
    def _(q):
        part = mm(v_all[rows_of(q, step_rows)], tall[...].reshape(d_all, own))
        sens[rows_of(q, step_rows)] = ((2.0 / row_count) * part).astype(bf16)

    def finish(rel):
        q = at_z(rel)
        acc[...] += mm(xc_all[q], sens[rows_of(q, own)])

    finish(0)
    for dist in range(1, half):
        if dist > 2:
            all_in(1, dist)
            center(zn - dist)
            center(dist)
        finish(zn - dist)
        finish(dist)
    all_in(1, half)
    center(half)
    q = at_z(half)
    o_ref[...] = (acc[...] + mm(xc_all[q], sens[rows_of(q, own)])).astype(bf16)

    pair.wait_send()
    for arr, full in ((0, g_all), (1, x_all)):
        arrived(full.at[pl.ds(0, zn - 1)], ring_s.at[arr])
    v_arrived(zn - 1, vr_s.at[0])
    v_arrived(sum((ny if y_first(rel) else nx) - 1 for rel in range(zn)), v1_s.at[0])
    v_arrived(sum(ny * (nx - 1) if y_first(rel) else nx * (ny - 1) for rel in range(zn)), v2_s.at[0])
    arrived(v_all.at[pl.ds(0, d_all // 2)], vd.at[0])
    v_arrived(zn - 1, vo.at[0])
    arrived(sums.at[pl.ds(0, n - 1)], su.at[0])
    arrived(means.at[pl.ds(0, zn - 1)], me_sem.at[0])
    for group in range(last + 1):
        arrived(parts.at[pl.ds(0, n - 1), :, group_lanes[group]], rs_sem.at[0, group])
        if len(sym_slots(group)):
            arrived(sym_bytes(group), sy_sem.at[0, group])
        arrived(s_view(group)(pl.ds(0, h - 1), core), ag_sem.at[0, group])
    arrived(t_view(pl.ds(0, h - 1), core), ag_sem.at[0, 3])
    for copy in passes:
        copy.wait_send()
    arrived(yall.at[pl.ds(0, zn - 1)], ya_sem.at[0])


def local(features, grad_out, eigvecs, eigvals, whiten):
    tok, own = features.shape
    n, zn = lax.axis_size("rows"), lax.axis_size("feat")
    d_all = eigvals.shape[0]
    nar, rp = d_all // n, own // n
    h, half = n // 2, zn // 2
    row_count = tok * n
    scratch = [
        pltpu.VMEM((tok, own), bf16),
        pltpu.VMEM((tok, own), bf16),
        pltpu.VMEM((nar, own), f32),
        pltpu.VMEM((1, d_all), f32),
        pltpu.VMEM((d_all, own), bf16),
        pltpu.VMEM((zn, tok, own), bf16),
        pltpu.VMEM((zn, tok, own), bf16),
        pltpu.VMEM((zn, tok, own), bf16),
        pltpu.VMEM((d_all, d_all), bf16),
        pltpu.VMEM((d_all, 2 * nar), bf16),
        pltpu.VMEM((2, nar, own), bf16),
        pltpu.VMEM((own, tok), bf16),
        pltpu.VMEM((tok, own), bf16),
        pltpu.VMEM((tok, own), f32),
        pltpu.VMEM((n, 8, own), f32),
        pltpu.VMEM((8, own), f32),
        pltpu.VMEM((zn, 8, own), f32),
        pltpu.VMEM((n, rp, d_all), bf16),
        pltpu.VMEM((n, rp, d_all), bf16),
        pltpu.VMEM((zn, rp, own), bf16),
        pltpu.VMEM((zn, rp, own), bf16),
        pltpu.VMEM((rp, d_all), bf16),
        pltpu.VMEM((h, 2, rp, d_all), bf16),
        pltpu.VMEM((2 * nar, d_all), bf16),
        pltpu.VMEM((nar, own), f32),
        pltpu.VMEM((nar, own), bf16),
        pltpu.VMEM((zn, nar, own), bf16),
        pltpu.VMEM((nar, d_all), f32),
        pltpu.VMEM((nar, d_all), bf16),
        pltpu.VMEM((nar, own), bf16),
        pltpu.VMEM((h, 2, nar, own), bf16),
        pltpu.VMEM((d_all, own), bf16),
    ]
    dma = pltpu.SemaphoreType.DMA
    scratch += [dma((5,)), dma((2,)), dma((2, half, CHUNKS[0])), dma((2, half, CHUNKS[1])), dma((1,)), dma((2, half)), dma((2,))]
    scratch += [dma((1,)), dma((zn,)), dma((1,)), dma((zn,)), dma((2,)), dma((2,)), dma((2,)), dma((2,))]
    scratch += [dma((2, 3)), dma((2, 3)), dma((2, 4)), dma((2, 4)), dma((2,))]
    hbm = pl.BlockSpec(memory_space=pl.ANY)
    return pl.pallas_call(
        functools.partial(body, n, zn, row_count),
        out_shape=pltpu.VMEM((tok, own), bf16),
        in_specs=[hbm] * 5,
        out_specs=VMEM,
        scratch_shapes=scratch,
        compiler_params=pltpu.CompilerParams(collective_id=1, has_side_effects=True, vmem_limit_bytes=58 * 2**20),
        cost_estimate=pl.CostEstimate(flops=8_000_000_000, bytes_accessed=16 * 2**20, transcendentals=0),
    )(features, grad_out, eigvecs.T, eigvals.reshape(1, d_all), whiten)


def solution(mesh):
    in_specs = (P("rows", "feat"), P("rows", "feat"), P("feat", "rows"), P(), P(None, "feat"))
    out_specs = P("rows", "feat")
    return jax.shard_map(local, mesh=mesh, in_specs=in_specs, out_specs=out_specs, check_vma=False)
```

```python
import functools
import math

import jax
import jax.numpy as jnp
from jax import lax
from jax.experimental import pallas as pl
from jax.experimental.pallas import tpu as pltpu
from jax.sharding import PartitionSpec as P

MESH = pl.DeviceIdType.MESH
VMEM = pl.BlockSpec(memory_space=pltpu.VMEM)
bf16, f32 = jnp.bfloat16, jnp.float32
CHUNKS = (4, 4)


def remote(src, dst, send, recv, axis, target):
    return pltpu.make_async_remote_copy(
        src_ref=src, dst_ref=dst, send_sem=send, recv_sem=recv,
        device_id={axis: target}, device_id_type=MESH,
    )


def lanes(index, width):
    return pl.ds(pl.multiple_of(index * width, width), width)


def mm(a, b, ca=1, cb=0):
    return lax.dot_general(a, b, (((ca,), (cb,)), ((), ())), preferred_element_type=f32)


def slot_order(zn):
    order = [0]
    for dist in range(1, zn // 2):
        order += [zn - dist, dist]
    return order + [zn // 2]


def body(n, zn, row_count, x_hbm, g_hbm, v_hbm, e_hbm, w_hbm, o_ref,
         x_ref, g_ref, v_ref, e_ref, w_ref, x_all, xc_all, g_all, v_all, v_col, v_pair, xct, gc, acc, sums, sums_own, means,
         pieces, parts, tile, rtile, spiece, sall, vct, yacc, yown, yall, kern, mt, town, tall, sens,
         ld, ring_s, ring_g, ring_x, vr_s, vr_r, vm, v1_s, v1_r, v2_s, v2_r, vd, vo, su, me_sem, rs_sem, sy_sem, ag_sem, am_sem, ya_sem):
    me, z = lax.axis_index("rows"), lax.axis_index("feat")
    core, chip = lax.rem(me, 2), me // 2
    mate = me + 1 - 2 * core
    h = n // 2
    nx = math.isqrt(h)
    ny = h // nx
    yy, xx = chip // nx, lax.rem(chip, nx)
    half = zn // 2
    tok, own = x_ref.shape
    d_all = v_all.shape[0]
    nar = d_all // n
    wide = 2 * nar
    hv = own // 2
    rp = own // n
    order = slot_order(zn)
    ring_r = (ring_g, ring_x)

    loads = []
    for i, (src, dst) in enumerate([(g_hbm, g_ref), (v_hbm, v_ref), (x_hbm, x_ref), (e_hbm, e_ref), (w_hbm, w_ref)]):
        load = pltpu.make_async_copy(src, dst, ld.at[i])
        load.start()
        loads.append(load)
    barrier = pltpu.get_barrier_semaphore()
    for d in range(1, n):
        pl.semaphore_signal(barrier, inc=1, device_id={"rows": lax.rem(me + d, n)}, device_id_type=MESH)
    for d in range(1, zn):
        pl.semaphore_signal(barrier, inc=1, device_id={"feat": lax.rem(z + d, zn)}, device_id_type=MESH)
    loads[0].wait()
    loads[1].wait()
    v_pair[core] = v_ref[...].astype(bf16)
    pl.semaphore_wait(barrier, n + zn - 2)

    def at_z(rel):
        return lax.rem(z + rel, zn)

    def rows_of(block, count):
        return pl.ds(pl.multiple_of(block * count, count), count)

    def arrived(ref, sem):
        pltpu.make_async_copy(ref, ref, sem).wait()

    def block_of(way, dist):
        return at_z(zn - dist) if way == 0 else at_z(dist)

    def next_of(way):
        return at_z(1) if way == 0 else at_z(zn - 1)

    def units(arr, step):
        return range(CHUNKS[arr] if step < half - 1 else CHUNKS[arr] // 2)

    def hop(arr, way, step, unit):
        full, mine = (g_all, g_ref) if arr == 0 else (x_all, x_ref)
        count = CHUNKS[arr]
        rows = pl.ds((unit + way * (count // 2)) % count * (tok // count), tok // count)
        there = full.at[block_of(way, step), rows]
        src = there if step else mine.at[rows]
        return remote(src, there, ring_s.at[arr], ring_r[arr].at[way, step, unit], "feat", next_of(way))

    def vpart(block, lane):
        return v_all.at[rows_of(2 * block + core, hv), lanes(lane, wide)]

    def v_mine(block):
        return v_col.at[rows_of(2 * block + core, hv)]

    def v_keep(block):
        rows = rows_of(2 * block + core, hv)
        v_all[rows, lanes(chip, wide)] = v_col[rows]

    def v_arrived(count, sem):
        if count * wide > d_all:
            arrived(v_all.at[pl.ds(0, count * wide * hv // d_all)], sem)
        elif count:
            arrived(v_all.at[pl.ds(0, hv), pl.ds(0, count * wide)], sem)

    def vhop(way, step):
        ref = v_mine(block_of(way, step))
        return remote(ref, ref, vr_s.at[0], vr_r.at[way, step], "feat", next_of(way))

    def y_first(rel):
        return rel == 0 or rel > half

    def by_y(d):
        return (lax.rem(yy + d, ny) * nx + xx) * 2 + core

    def by_x(d):
        return (yy * nx + lax.rem(xx + d, nx)) * 2 + core

    def v_first(rel):
        src, ref = v_mine(at_z(rel)), vpart(at_z(rel), chip)
        if rel:
            remote(src, src, vo.at[0], vo.at[1], "rows", mate).start()
        v_keep(at_z(rel))
        for d in range(1, ny if y_first(rel) else nx):
            target = by_y(d) if y_first(rel) else by_x(d)
            remote(src, ref, v1_s.at[0], v1_r.at[rel], "rows", target).start()

    def v_second(rel):
        v_arrived((ny if y_first(rel) else nx) - 1, v1_r.at[rel])
        if y_first(rel):
            for e in range(ny):
                ref = vpart(at_z(rel), lax.rem(yy + ny - e, ny) * nx + xx)
                src = ref if e else v_mine(at_z(rel))
                for d in range(1, nx):
                    remote(src, ref, v2_s.at[0], v2_r.at[rel], "rows", by_x(d)).start()
        else:
            ref = v_all.at[rows_of(2 * at_z(rel) + core, hv), lanes(yy, nx * wide)]
            for d in range(1, ny):
                remote(ref, ref, v2_s.at[0], v2_r.at[rel], "rows", by_y(d)).start()

    def v_third(rel):
        v_arrived(ny * (nx - 1) if y_first(rel) else nx * (ny - 1), v2_r.at[rel])
        ref = v_all.at[rows_of(2 * at_z(rel) + core, hv)]
        remote(ref, ref, vd.at[0], vd.at[1], "rows", mate).start()

    for way in (0, 1):
        hop(0, way, 0, 0).start()
    pair = remote(v_pair.at[core], v_pair.at[core], vm.at[0], vm.at[1], "rows", mate)
    pair.start()
    loads[2].wait()
    sums_own[0:1] = jnp.sum(x_ref[...].astype(f32), axis=0, keepdims=True)
    sums_own[1:2] = jnp.sum(g_ref[...].astype(f32), axis=0, keepdims=True)
    pair.wait_recv()
    both = jnp.concatenate([v_pair[0].astype(f32), v_pair[1].astype(f32)], axis=0)
    v_col[rows_of(z, own)] = both.T.astype(bf16)
    for way in (0, 1):
        if way == 0 or half > 1:
            vhop(way, 0).start()
        for unit in units(0, 0)[1:]:
            hop(0, way, 0, unit).start()
    for d in range(1, n):
        remote(sums_own, sums.at[me], su.at[0], su.at[1], "rows", lax.rem(me + d, n)).start()
    sums[me] = sums_own[...]
    v_first(0)

    loads[3].wait()
    root = jnp.sqrt(e_ref[...])
    shape = (nar, d_all)
    wanted = me * nar + lax.broadcasted_iota(jnp.int32, shape, 0)
    hit = wanted == lax.broadcasted_iota(jnp.int32, shape, 1)
    root_row = jnp.sum(jnp.where(hit, jnp.broadcast_to(root, shape), 0.0), axis=1, keepdims=True)
    kern[...] = -1.0 / ((root_row * root) * (root_row + root))

    arrived(sums.at[pl.ds(0, n - 1)], su.at[1])
    means[z] = jnp.sum(sums[...], axis=0) / row_count
    for d in range(1, zn):
        remote(means.at[z], means.at[z], me_sem.at[0], me_sem.at[1], "feat", at_z(d)).start()
    xc = x_ref[...].astype(f32) - means[z, 0:1]
    xc_all[z] = xc.astype(bf16)
    xct[...] = xc.T.astype(bf16)
    loads[4].wait()

    def gram(slot):
        rel = order[slot]
        q = at_z(rel)
        src = g_ref if rel == 0 else g_all.at[q]
        gc[...] = (src[...].astype(f32) - means[q, 1:2]).astype(bf16)
        block = mm(xct[...], gc[...])
        lane = pl.ds(slot * own, own)

        def put(value):
            pieces[:, :, lane] = value.reshape(n, rp, own).astype(bf16)

        if rel == 0:
            put(0.5 * (block + block.T))
        else:
            @pl.when(z < q)
            def _():
                put(0.5 * block)

            @pl.when(z > q)
            def _():
                put(0.5 * block.T)

    def product(slot):
        gw = mm(gc[...], w_ref[rows_of(at_z(order[slot]), own)])
        acc[...] = gw if slot == 0 else acc[...] + gw

    split = max(1, zn - 3)
    groups = [(lo, hi) for lo, hi in ((0, split), (split, zn - 1), (zn - 1, zn)) if lo < hi]
    last = len(groups) - 1
    group_lanes = [pl.ds(lo * own, (hi - lo) * own) for lo, hi in groups]

    def rs_start(group):
        lane = group_lanes[group]
        for d in range(1, n):
            s = lax.rem(me + d, n)
            remote(pieces.at[s, :, lane], parts.at[me, :, lane], rs_sem.at[0, group], rs_sem.at[1, group], "rows", s).start()

    def rs_sum(group):
        (lo, hi), lane = groups[group], group_lanes[group]
        arrived(parts.at[pl.ds(0, n - 1), :, lane], rs_sem.at[1, group])
        total = pieces[me, :, lane].astype(f32)
        for d in range(1, n):
            total = total + parts[lax.rem(me + n - d, n), :, lane].astype(f32)
        for slot in range(lo, hi):
            tile[slot] = total[:, (slot - lo) * own:(slot - lo + 1) * own].astype(bf16)

    def sym_slots(group):
        return range(max(1, groups[group][0]), groups[group][1])

    def sym_start(group):
        for slot in sym_slots(group):
            d = order[slot]
            there = rtile.at[order.index((zn - d) % zn)]
            remote(tile.at[slot], there, sy_sem.at[0, group], sy_sem.at[1, group], "feat", at_z(d)).start()

    def sym_bytes(group):
        return rtile.at[pl.ds(sym_slots(group)[0], len(sym_slots(group)))]

    def sym_end(group):
        if len(sym_slots(group)):
            arrived(sym_bytes(group), sy_sem.at[1, group])
        lo, hi = groups[group]
        for slot in range(lo, hi):
            both = tile[slot].astype(f32)
            if slot:
                both = both + rtile[slot].astype(f32)
            spiece[:, pl.ds(slot * own, own)] = both.astype(bf16)

    def gather_start(which, src, view):
        for d in range(1, h):
            there = lax.rem(chip + d, h)
            remote(src, view(chip, core), ag_sem.at[0, which], ag_sem.at[1, which], "rows", 2 * there + core).start()

    def gather_pass(which, view):
        arrived(view(pl.ds(0, h - 1), core), ag_sem.at[1, which])
        mine = view(pl.ds(0, h), core)
        copy = remote(mine, mine, am_sem.at[0, which], am_sem.at[1, which], "rows", mate)
        copy.start()
        return copy

    def s_view(group):
        return lambda chips, side: sall.at[chips, side, :, group_lanes[group]]

    def t_view(chips, side):
        return tall.at[chips, side]

    done = set()

    def take(arr, way, step, unit):
        if (arr, way, step, unit) not in done:
            done.add((arr, way, step, unit))
            hop(arr, way, step, unit).wait_recv()

    forwards = [(step, unit) for step in range(half) for unit in units(1, step)]
    state = {"next": 0}

    def pump(count):
        for _ in range(count):
            if state["next"] < len(forwards):
                step, unit = forwards[state["next"]]
                state["next"] += 1
                for way in (0, 1):
                    if step:
                        take(1, way, step - 1, unit)
                    hop(1, way, step, unit).start()

    def all_in(arr, dist):
        for unit in units(arr, dist - 1):
            for way in (0, 1):
                take(arr, way, dist - 1, unit)

    def center(rel):
        q = at_z(rel)
        xc_all[q] = (x_all[q].astype(f32) - means[q, 0:1]).astype(bf16)

    gram(0)
    if split == 1:
        rs_start(0)
    product(0)
    v_second(0)
    rels = [[0]]
    for dist in range(1, half + 1):
        got = []
        for way in (0, 1):
            if way == 0 or dist < half:
                vhop(way, dist - 1).wait_recv()
                if (way == 0 and dist < half) or (way == 1 and dist < half - 1):
                    vhop(way, dist).start()
                rel = zn - dist if way == 0 else dist
                v_first(rel)
                got.append(rel)
        rels.append(got)
        for unit in units(0, dist - 1):
            for way in (0, 1):
                take(0, way, dist - 1, unit)
                if dist < half and unit in units(0, dist):
                    hop(0, way, dist, unit).start()
            if dist == half - 1 and unit == 1:
                rs_sum(0)
                sym_start(0)
            if dist == half - 1 and unit == 3:
                pump(1)
            if dist == half:
                pump(1 - unit)
            if dist >= 2 and unit == 1:
                for rel in rels[dist - 2]:
                    v_third(rel)
        if dist == 1:
            arrived(means.at[pl.ds(0, zn - 1)], me_sem.at[1])
        mine = [slot for slot in range(zn) if order[slot] in (dist, zn - dist)]
        for slot in mine:
            gram(slot)
            for group in range(last):
                if slot == groups[group][1] - 1:
                    rs_start(group)
            if dist < half:
                product(slot)
        if dist < half - 1:
            for rel in rels[dist]:
                v_second(rel)
    def s_start(group):
        sym_end(group)
        lane = group_lanes[group]
        sall[chip, core, :, lane] = spiece[:, lane]
        gather_start(group, spiece.at[:, lane], s_view(group))

    rs_start(last)
    product(zn - 1)
    if half == 1:
        rs_sum(0)
        sym_start(0)
    s_start(0)
    if half > 1:
        for rel in rels[half - 1]:
            v_second(rel)
    for group in range(1, last):
        rs_sum(group)
        sym_start(group)
    pump(1)
    rs_sum(last)
    sym_start(last)
    pump(1)
    passes = [gather_pass(0, s_view(0))] if last else []
    for group in range(1, last):
        s_start(group)
    pump(1)
    s_start(last)
    for rel in rels[half]:
        v_second(rel)
    pump(2)
    v_arrived(zn - 1, vo.at[1])
    vct[...] = v_col[...].astype(f32).T.astype(bf16)
    yacc[...] = jnp.zeros_like(yacc)

    def y_part(group):
        passes[group].wait_recv()
        lo, hi = groups[group]
        for slot in range(lo, hi):
            q = at_z(order[slot])
            block = sall[:, :, :, pl.ds(slot * own, own)].astype(f32).reshape(own, own).astype(bf16)
            left = vct[rows_of(core, nar), lanes(q, own)]
            if slot == 0:
                yacc[...] += mm(left, block)
            else:
                @pl.when(q < z)
                def _():
                    yacc[...] += mm(left, block)

                @pl.when(q > z)
                def _():
                    yacc[...] += mm(left, block, 1, 1)

    if last:
        y_part(0)
    for group in range(1, last + 1):
        passes.append(gather_pass(group, s_view(group)))
    if not last:
        passes.append(gather_pass(0, s_view(0)))
    pump(1)
    for group in range(1 if last else 0, last + 1):
        y_part(group)
    yown[...] = yacc[...].astype(bf16)
    for d in range(1, zn):
        remote(yown, yall.at[z], ya_sem.at[0], ya_sem.at[1], "feat", at_z(d)).start()
    yall[z] = yown[...]
    for rel in rels[half - 1] + rels[half]:
        v_third(rel)
    pump(1)
    if half > 1:
        all_in(1, 1)
        center(zn - 1)
        center(1)
    arrived(yall.at[pl.ds(0, zn - 1)], ya_sem.at[1])
    pump(2)
    arrived(v_all.at[pl.ds(0, d_all // 2)], vd.at[1])
    left = jnp.concatenate([yall[q] for q in range(zn)], axis=1)
    mt[...] = (kern[...] * mm(left, v_all[...])).astype(bf16)
    town[...] = mm(mt[...], v_all[rows_of(z, own)], 1, 1).astype(bf16)
    tall[chip, core] = town[...]
    gather_start(3, town, t_view)
    pump(2)
    if half > 2:
        all_in(1, 2)
        center(zn - 2)
        center(2)
    pump(1)
    passes.append(gather_pass(3, t_view))
    pump(len(forwards))
    passes[-1].wait_recv()
    step_rows = d_all // 4

    @pl.loop(0, 4)
    def _(q):
        part = mm(v_all[rows_of(q, step_rows)], tall[...].reshape(d_all, own))
        sens[rows_of(q, step_rows)] = ((2.0 / row_count) * part).astype(bf16)

    def finish(rel):
        q = at_z(rel)
        acc[...] += mm(xc_all[q], sens[rows_of(q, own)])

    finish(0)
    for dist in range(1, half):
        if dist > 2:
            all_in(1, dist)
            center(zn - dist)
            center(dist)
        finish(zn - dist)
        finish(dist)
    all_in(1, half)
    center(half)
    q = at_z(half)
    o_ref[...] = (acc[...] + mm(xc_all[q], sens[rows_of(q, own)])).astype(bf16)

    pair.wait_send()
    for arr, full in ((0, g_all), (1, x_all)):
        arrived(full.at[pl.ds(0, zn - 1)], ring_s.at[arr])
    v_arrived(zn - 1, vr_s.at[0])
    v_arrived(sum((ny if y_first(rel) else nx) - 1 for rel in range(zn)), v1_s.at[0])
    v_arrived(sum(ny * (nx - 1) if y_first(rel) else nx * (ny - 1) for rel in range(zn)), v2_s.at[0])
    arrived(v_all.at[pl.ds(0, d_all // 2)], vd.at[0])
    v_arrived(zn - 1, vo.at[0])
    arrived(sums.at[pl.ds(0, n - 1)], su.at[0])
    arrived(means.at[pl.ds(0, zn - 1)], me_sem.at[0])
    for group in range(last + 1):
        arrived(parts.at[pl.ds(0, n - 1), :, group_lanes[group]], rs_sem.at[0, group])
        if len(sym_slots(group)):
            arrived(sym_bytes(group), sy_sem.at[0, group])
        arrived(s_view(group)(pl.ds(0, h - 1), core), ag_sem.at[0, group])
    arrived(t_view(pl.ds(0, h - 1), core), ag_sem.at[0, 3])
    for copy in passes:
        copy.wait_send()
    arrived(yall.at[pl.ds(0, zn - 1)], ya_sem.at[0])


def local(features, grad_out, eigvecs, eigvals, whiten):
    tok, own = features.shape
    n, zn = lax.axis_size("rows"), lax.axis_size("feat")
    d_all = eigvals.shape[0]
    nar, rp = d_all // n, own // n
    h, half = n // 2, zn // 2
    row_count = tok * n
    scratch = [
        pltpu.VMEM((tok, own), bf16),
        pltpu.VMEM((tok, own), bf16),
        pltpu.VMEM((nar, own), f32),
        pltpu.VMEM((1, d_all), f32),
        pltpu.VMEM((d_all, own), bf16),
        pltpu.VMEM((zn, tok, own), bf16),
        pltpu.VMEM((zn, tok, own), bf16),
        pltpu.VMEM((zn, tok, own), bf16),
        pltpu.VMEM((d_all, d_all), bf16),
        pltpu.VMEM((d_all, 2 * nar), bf16),
        pltpu.VMEM((2, nar, own), bf16),
        pltpu.VMEM((own, tok), bf16),
        pltpu.VMEM((tok, own), bf16),
        pltpu.VMEM((tok, own), f32),
        pltpu.VMEM((n, 2, own), f32),
        pltpu.VMEM((2, own), f32),
        pltpu.VMEM((zn, 2, own), f32),
        pltpu.VMEM((n, rp, d_all), bf16),
        pltpu.VMEM((n, rp, d_all), bf16),
        pltpu.VMEM((zn, rp, own), bf16),
        pltpu.VMEM((zn, rp, own), bf16),
        pltpu.VMEM((rp, d_all), bf16),
        pltpu.VMEM((h, 2, rp, d_all), bf16),
        pltpu.VMEM((2 * nar, d_all), bf16),
        pltpu.VMEM((nar, own), f32),
        pltpu.VMEM((nar, own), bf16),
        pltpu.VMEM((zn, nar, own), bf16),
        pltpu.VMEM((nar, d_all), f32),
        pltpu.VMEM((nar, d_all), bf16),
        pltpu.VMEM((nar, own), bf16),
        pltpu.VMEM((h, 2, nar, own), bf16),
        pltpu.VMEM((d_all, own), bf16),
    ]
    dma = pltpu.SemaphoreType.DMA
    scratch += [dma((5,)), dma((2,)), dma((2, half, CHUNKS[0])), dma((2, half, CHUNKS[1])), dma((1,)), dma((2, half)), dma((2,))]
    scratch += [dma((1,)), dma((zn,)), dma((1,)), dma((zn,)), dma((2,)), dma((2,)), dma((2,)), dma((2,))]
    scratch += [dma((2, 3)), dma((2, 3)), dma((2, 4)), dma((2, 4)), dma((2,))]
    hbm = pl.BlockSpec(memory_space=pl.ANY)
    return pl.pallas_call(
        functools.partial(body, n, zn, row_count),
        out_shape=pltpu.VMEM((tok, own), bf16),
        in_specs=[hbm] * 5,
        out_specs=VMEM,
        scratch_shapes=scratch,
        compiler_params=pltpu.CompilerParams(collective_id=1, has_side_effects=True, vmem_limit_bytes=58 * 2**20),
        cost_estimate=pl.CostEstimate(flops=8_000_000_000, bytes_accessed=16 * 2**20, transcendentals=0),
    )(features, grad_out, eigvecs.T, eigvals.reshape(1, d_all), whiten)


def solution(mesh):
    in_specs = (P("rows", "feat"), P("rows", "feat"), P("feat", "rows"), P(), P(None, "feat"))
    out_specs = P("rows", "feat")
    return jax.shard_map(local, mesh=mesh, in_specs=in_specs, out_specs=out_specs, check_vma=False)
```

```python
import functools
import math

import jax
import jax.numpy as jnp
from jax import lax
from jax.experimental import pallas as pl
from jax.experimental.pallas import tpu as pltpu
from jax.sharding import PartitionSpec as P

MESH = pl.DeviceIdType.MESH
VMEM = pl.BlockSpec(memory_space=pltpu.VMEM)
bf16, f32 = jnp.bfloat16, jnp.float32
CHUNKS = (4, 4)


def remote(src, dst, send, recv, axis, target):
    return pltpu.make_async_remote_copy(
        src_ref=src, dst_ref=dst, send_sem=send, recv_sem=recv,
        device_id={axis: target}, device_id_type=MESH,
    )


def lanes(index, width):
    return pl.ds(pl.multiple_of(index * width, width), width)


def mm(a, b, ca=1, cb=0):
    return lax.dot_general(a, b, (((ca,), (cb,)), ((), ())), preferred_element_type=f32)


def slot_order(zn):
    order = [0]
    for dist in range(1, zn // 2):
        order += [zn - dist, dist]
    return order + [zn // 2]


def body(n, zn, row_count, x_hbm, g_hbm, v_hbm, e_hbm, w_hbm, o_ref,
         x_ref, g_ref, v_ref, e_ref, w_ref, x_all, xc_all, g_all, v_all, v_col, v_pair, xct, gc, acc, sums, sums_own, means,
         pieces, parts, tile, rtile, spiece, sall, vct, yacc, yown, yall, kern, mt, tout, tin, town, tall, sens, xv, xvb,
         ld, ring_s, ring_g, ring_x, vr_s, vr_r, vm, v1_s, v1_r, v2_s, v2_r, vd, vo, su, me_sem, rs_sem, sy_sem, ag_sem, am_sem, ya_sem, tz_sem):
    me, z = lax.axis_index("rows"), lax.axis_index("feat")
    core, chip = lax.rem(me, 2), me // 2
    mate = me + 1 - 2 * core
    h = n // 2
    nx = math.isqrt(h)
    ny = h // nx
    yy, xx = chip // nx, lax.rem(chip, nx)
    half = zn // 2
    tok, own = x_ref.shape
    d_all = v_all.shape[0]
    nar = d_all // n
    wide = 2 * nar
    hv = own // 2
    rp = own // n
    order = slot_order(zn)
    ring_r = (ring_g, ring_x)

    loads = []
    for i, (src, dst) in enumerate([(g_hbm, g_ref), (v_hbm, v_ref), (x_hbm, x_ref), (e_hbm, e_ref), (w_hbm, w_ref)]):
        load = pltpu.make_async_copy(src, dst, ld.at[i])
        load.start()
        loads.append(load)
    barrier = pltpu.get_barrier_semaphore()
    for d in range(1, n):
        pl.semaphore_signal(barrier, inc=1, device_id={"rows": lax.rem(me + d, n)}, device_id_type=MESH)
    for d in range(1, zn):
        pl.semaphore_signal(barrier, inc=1, device_id={"feat": lax.rem(z + d, zn)}, device_id_type=MESH)
    loads[0].wait()
    loads[1].wait()
    v_pair[core] = v_ref[...].astype(bf16)
    pl.semaphore_wait(barrier, n + zn - 2)

    def at_z(rel):
        return lax.rem(z + rel, zn)

    def rows_of(block, count):
        return pl.ds(pl.multiple_of(block * count, count), count)

    def arrived(ref, sem):
        pltpu.make_async_copy(ref, ref, sem).wait()

    def block_of(way, dist):
        return at_z(zn - dist) if way == 0 else at_z(dist)

    def next_of(way):
        return at_z(1) if way == 0 else at_z(zn - 1)

    def units(arr, step):
        return range(CHUNKS[arr] if step < half - 1 else CHUNKS[arr] // 2)

    def hop(arr, way, step, unit):
        full, mine = (g_all, g_ref) if arr == 0 else (x_all, x_ref)
        count = CHUNKS[arr]
        rows = pl.ds((unit + way * (count // 2)) % count * (tok // count), tok // count)
        there = full.at[block_of(way, step), rows]
        src = there if step else mine.at[rows]
        return remote(src, there, ring_s.at[arr], ring_r[arr].at[way, step, unit], "feat", next_of(way))

    def vpart(block, lane):
        return v_all.at[rows_of(2 * block + core, hv), lanes(lane, wide)]

    def v_mine(block):
        return v_col.at[rows_of(2 * block + core, hv)]

    def v_keep(block):
        rows = rows_of(2 * block + core, hv)
        v_all[rows, lanes(chip, wide)] = v_col[rows]

    def v_arrived(count, sem):
        if count * wide > d_all:
            arrived(v_all.at[pl.ds(0, count * wide * hv // d_all)], sem)
        elif count:
            arrived(v_all.at[pl.ds(0, hv), pl.ds(0, count * wide)], sem)

    def vhop(way, step):
        ref = v_mine(block_of(way, step))
        return remote(ref, ref, vr_s.at[0], vr_r.at[way, step], "feat", next_of(way))

    def y_first(rel):
        return rel == 0 or rel > half

    def by_y(d):
        return (lax.rem(yy + d, ny) * nx + xx) * 2 + core

    def by_x(d):
        return (yy * nx + lax.rem(xx + d, nx)) * 2 + core

    def v_first(rel):
        src, ref = v_mine(at_z(rel)), vpart(at_z(rel), chip)
        if rel:
            remote(src, src, vo.at[0], vo.at[1], "rows", mate).start()
        v_keep(at_z(rel))
        for d in range(1, ny if y_first(rel) else nx):
            target = by_y(d) if y_first(rel) else by_x(d)
            remote(src, ref, v1_s.at[0], v1_r.at[rel], "rows", target).start()

    def v_second(rel):
        v_arrived((ny if y_first(rel) else nx) - 1, v1_r.at[rel])
        if y_first(rel):
            for e in range(ny):
                ref = vpart(at_z(rel), lax.rem(yy + ny - e, ny) * nx + xx)
                src = ref if e else v_mine(at_z(rel))
                for d in range(1, nx):
                    remote(src, ref, v2_s.at[0], v2_r.at[rel], "rows", by_x(d)).start()
        else:
            ref = v_all.at[rows_of(2 * at_z(rel) + core, hv), lanes(yy, nx * wide)]
            for d in range(1, ny):
                remote(ref, ref, v2_s.at[0], v2_r.at[rel], "rows", by_y(d)).start()

    def v_third(rel):
        v_arrived(ny * (nx - 1) if y_first(rel) else nx * (ny - 1), v2_r.at[rel])
        ref = v_all.at[rows_of(2 * at_z(rel) + core, hv)]
        remote(ref, ref, vd.at[0], vd.at[1], "rows", mate).start()

    for way in (0, 1):
        hop(0, way, 0, 0).start()
    pair = remote(v_pair.at[core], v_pair.at[core], vm.at[0], vm.at[1], "rows", mate)
    pair.start()
    loads[2].wait()
    sums_own[0:1] = jnp.sum(x_ref[...].astype(f32), axis=0, keepdims=True)
    sums_own[1:2] = jnp.sum(g_ref[...].astype(f32), axis=0, keepdims=True)
    pair.wait_recv()
    both = jnp.concatenate([v_pair[0].astype(f32), v_pair[1].astype(f32)], axis=0)
    v_col[rows_of(z, own)] = both.T.astype(bf16)
    for way in (0, 1):
        if way == 0 or half > 1:
            vhop(way, 0).start()
        for unit in units(0, 0)[1:]:
            hop(0, way, 0, unit).start()
    for d in range(1, n):
        remote(sums_own, sums.at[me], su.at[0], su.at[1], "rows", lax.rem(me + d, n)).start()
    sums[me] = sums_own[...]
    v_first(0)

    loads[3].wait()
    root = jnp.sqrt(e_ref[...])
    shape = (nar // zn, d_all)
    wanted = me * nar + z * (nar // zn) + lax.broadcasted_iota(jnp.int32, shape, 0)
    hit = wanted == lax.broadcasted_iota(jnp.int32, shape, 1)
    root_row = jnp.sum(jnp.where(hit, jnp.broadcast_to(root, shape), 0.0), axis=1, keepdims=True)
    kern[...] = -1.0 / ((root_row * root) * (root_row + root))

    arrived(sums.at[pl.ds(0, n - 1)], su.at[1])
    means[z] = jnp.sum(sums[...], axis=0) / row_count
    for d in range(1, zn):
        remote(means.at[z], means.at[z], me_sem.at[0], me_sem.at[1], "feat", at_z(d)).start()
    xc = x_ref[...].astype(f32) - means[z, 0:1]
    xc_all[z] = xc.astype(bf16)
    xct[...] = xc.T.astype(bf16)
    loads[4].wait()

    def gram(slot):
        rel = order[slot]
        q = at_z(rel)
        src = g_ref if rel == 0 else g_all.at[q]
        gc[...] = (src[...].astype(f32) - means[q, 1:2]).astype(bf16)
        block = mm(xct[...], gc[...])
        lane = pl.ds(slot * own, own)

        def put(value):
            pieces[:, :, lane] = value.reshape(n, rp, own).astype(bf16)

        if rel == 0:
            put(0.5 * (block + block.T))
        else:
            @pl.when(z < q)
            def _():
                put(0.5 * block)

            @pl.when(z > q)
            def _():
                put(0.5 * block.T)

    def product(slot):
        gw = mm(gc[...], w_ref[rows_of(at_z(order[slot]), own)])
        acc[...] = gw if slot == 0 else acc[...] + gw

    split = max(1, zn - 3)
    groups = [(lo, hi) for lo, hi in ((0, split), (split, zn - 1), (zn - 1, zn)) if lo < hi]
    last = len(groups) - 1
    group_lanes = [pl.ds(lo * own, (hi - lo) * own) for lo, hi in groups]

    def rs_start(group):
        lane = group_lanes[group]
        for d in range(1, n):
            s = lax.rem(me + d, n)
            remote(pieces.at[s, :, lane], parts.at[me, :, lane], rs_sem.at[0, group], rs_sem.at[1, group], "rows", s).start()

    def rs_sum(group):
        (lo, hi), lane = groups[group], group_lanes[group]
        arrived(parts.at[pl.ds(0, n - 1), :, lane], rs_sem.at[1, group])
        total = pieces[me, :, lane].astype(f32)
        for d in range(1, n):
            total = total + parts[lax.rem(me + n - d, n), :, lane].astype(f32)
        for slot in range(lo, hi):
            tile[slot] = total[:, (slot - lo) * own:(slot - lo + 1) * own].astype(bf16)

    def sym_slots(group):
        return range(max(1, groups[group][0]), groups[group][1])

    def sym_start(group):
        for slot in sym_slots(group):
            d = order[slot]
            there = rtile.at[order.index((zn - d) % zn)]
            remote(tile.at[slot], there, sy_sem.at[0, group], sy_sem.at[1, group], "feat", at_z(d)).start()

    def sym_bytes(group):
        return rtile.at[pl.ds(sym_slots(group)[0], len(sym_slots(group)))]

    def sym_end(group):
        if len(sym_slots(group)):
            arrived(sym_bytes(group), sy_sem.at[1, group])
        lo, hi = groups[group]
        for slot in range(lo, hi):
            both = tile[slot].astype(f32)
            if slot:
                both = both + rtile[slot].astype(f32)
            spiece[:, pl.ds(slot * own, own)] = both.astype(bf16)

    def gather_start(which, src, view):
        for d in range(1, h):
            there = lax.rem(chip + d, h)
            remote(src, view(chip, core), ag_sem.at[0, which], ag_sem.at[1, which], "rows", 2 * there + core).start()

    def gather_pass(which, view):
        arrived(view(pl.ds(0, h - 1), core), ag_sem.at[1, which])
        mine = view(pl.ds(0, h), core)
        copy = remote(mine, mine, am_sem.at[0, which], am_sem.at[1, which], "rows", mate)
        copy.start()
        return copy

    def s_view(group):
        return lambda chips, side: sall.at[chips, side, :, group_lanes[group]]

    def t_view(chips, side):
        return tall.at[chips, side]

    done = set()

    def take(arr, way, step, unit):
        if (arr, way, step, unit) not in done:
            done.add((arr, way, step, unit))
            hop(arr, way, step, unit).wait_recv()

    forwards = [(step, unit) for step in range(half) for unit in units(1, step)]
    state = {"next": 0}

    def pump(count):
        for _ in range(count):
            if state["next"] < len(forwards):
                step, unit = forwards[state["next"]]
                state["next"] += 1
                for way in (0, 1):
                    if step:
                        take(1, way, step - 1, unit)
                    hop(1, way, step, unit).start()

    def all_in(arr, dist):
        for unit in units(arr, dist - 1):
            for way in (0, 1):
                take(arr, way, dist - 1, unit)

    def center(rel):
        q = at_z(rel)
        xc_all[q] = (x_all[q].astype(f32) - means[q, 0:1]).astype(bf16)

    gram(0)
    if split == 1:
        rs_start(0)
    product(0)
    v_second(0)
    rels = [[0]]
    for dist in range(1, half + 1):
        got = []
        for way in (0, 1):
            if way == 0 or dist < half:
                vhop(way, dist - 1).wait_recv()
                if (way == 0 and dist < half) or (way == 1 and dist < half - 1):
                    vhop(way, dist).start()
                rel = zn - dist if way == 0 else dist
                v_first(rel)
                got.append(rel)
        rels.append(got)
        for unit in units(0, dist - 1):
            for way in (0, 1):
                take(0, way, dist - 1, unit)
                if dist < half and unit in units(0, dist):
                    hop(0, way, dist, unit).start()
            if dist == half - 1 and unit == 1:
                rs_sum(0)
                sym_start(0)
            if dist == half - 1 and unit == 3:
                pump(1)
            if dist == half:
                pump(1 - unit)
            if dist >= 2 and unit == 1:
                for rel in rels[dist - 2]:
                    v_third(rel)
        if dist == 1:
            arrived(means.at[pl.ds(0, zn - 1)], me_sem.at[1])
        mine = [slot for slot in range(zn) if order[slot] in (dist, zn - dist)]
        for slot in mine:
            gram(slot)
            for group in range(last):
                if slot == groups[group][1] - 1:
                    rs_start(group)
            if dist < half:
                product(slot)
        if dist < half - 1:
            for rel in rels[dist]:
                v_second(rel)
    def s_start(group):
        sym_end(group)
        lane = group_lanes[group]
        sall[chip, core, :, lane] = spiece[:, lane]
        gather_start(group, spiece.at[:, lane], s_view(group))

    rs_start(last)
    product(zn - 1)
    if half == 1:
        rs_sum(0)
        sym_start(0)
    s_start(0)
    if half > 1:
        for rel in rels[half - 1]:
            v_second(rel)
    for group in range(1, last):
        rs_sum(group)
        sym_start(group)
    pump(1)
    rs_sum(last)
    sym_start(last)
    pump(1)
    passes = [gather_pass(0, s_view(0))] if last else []
    for group in range(1, last):
        s_start(group)
    pump(1)
    s_start(last)
    for rel in rels[half]:
        v_second(rel)
    pump(2)
    v_arrived(zn - 1, vo.at[1])
    vct[...] = v_col[...].astype(f32).T.astype(bf16)
    yacc[...] = jnp.zeros_like(yacc)

    def y_part(group):
        passes[group].wait_recv()
        lo, hi = groups[group]
        for slot in range(lo, hi):
            q = at_z(order[slot])
            block = sall[:, :, :, pl.ds(slot * own, own)].astype(f32).reshape(own, own).astype(bf16)
            left = vct[rows_of(core, nar), lanes(q, own)]
            if slot == 0:
                yacc[...] += mm(left, block)
            else:
                @pl.when(q < z)
                def _():
                    yacc[...] += mm(left, block)

                @pl.when(q > z)
                def _():
                    yacc[...] += mm(left, block, 1, 1)

    if last:
        y_part(0)
    for group in range(1, last + 1):
        passes.append(gather_pass(group, s_view(group)))
    if not last:
        passes.append(gather_pass(0, s_view(0)))
    pump(0)
    for group in range(1 if last else 0, last + 1):
        y_part(group)
    yown[...] = yacc[...].reshape(zn, nar // zn, own).astype(bf16)
    for d in range(1, zn):
        remote(yown.at[at_z(d)], yall.at[z], ya_sem.at[0], ya_sem.at[1], "feat", at_z(d)).start()
    yall[z] = yown[z]
    for rel in rels[half - 1] + rels[half]:
        v_third(rel)
    pump(1)
    if half > 1:
        all_in(1, 1)
        center(zn - 1)
        center(1)

    def early(rels, first, final):
        rows_each = tok // 4

        @pl.loop(0, 4)
        def _(i):
            rows = rows_of(i, rows_each)
            total = 0.0 if first else xv[rows]
            for rel in rels:
                q = at_z(rel)
                total = total + mm(xc_all[q, rows], v_all[rows_of(q, own)])
            if final:
                xvb[rows] = total.astype(bf16)
            else:
                xv[rows] = total

    arrived(yall.at[pl.ds(0, zn - 1)], ya_sem.at[1])
    pump(1)
    arrived(v_all.at[pl.ds(0, d_all // 2)], vd.at[1])
    left = jnp.concatenate([yall[q] for q in range(zn)], axis=1)
    mt[...] = (kern[...] * mm(left, v_all[...])).astype(bf16)
    t_rows = mm(mt[...], v_all[...], 1, 1)
    for q in range(zn):
        tout[q] = t_rows[:, q * own:(q + 1) * own].astype(bf16)
    for d in range(1, zn):
        remote(tout.at[at_z(d)], tin.at[z], tz_sem.at[0], tz_sem.at[1], "feat", at_z(d)).start()
    tin[z] = tout[z]
    pump(2)
    early([0, zn - 1, 1] if half > 1 else [0], True, half <= 2)
    arrived(tin.at[pl.ds(0, zn - 1)], tz_sem.at[1])
    town[...] = tin[...].astype(f32).reshape(nar, own).astype(bf16)
    tall[chip, core] = town[...]
    gather_start(3, town, t_view)
    pump(2)
    for dist in range(2, half):
        if dist == half - 1:
            passes.append(gather_pass(3, t_view))
        all_in(1, dist)
        center(zn - dist)
        center(dist)
        early([zn - dist, dist], False, dist == half - 1)
        pump(1)
    if half <= 2:
        passes.append(gather_pass(3, t_view))
    pump(len(forwards))
    passes[-1].wait_recv()
    scale = 2.0 / row_count
    acc[...] += scale * mm(xvb[...], tall[...].reshape(d_all, own))
    last_rows = rows_of(at_z(half), own)
    sens[...] = (scale * mm(v_all[last_rows], tall[...].reshape(d_all, own))).astype(bf16)
    all_in(1, half)
    center(half)
    o_ref[...] = (acc[...] + mm(xc_all[at_z(half)], sens[...])).astype(bf16)

    pair.wait_send()
    for arr, full in ((0, g_all), (1, x_all)):
        arrived(full.at[pl.ds(0, zn - 1)], ring_s.at[arr])
    v_arrived(zn - 1, vr_s.at[0])
    v_arrived(sum((ny if y_first(rel) else nx) - 1 for rel in range(zn)), v1_s.at[0])
    v_arrived(sum(ny * (nx - 1) if y_first(rel) else nx * (ny - 1) for rel in range(zn)), v2_s.at[0])
    arrived(v_all.at[pl.ds(0, d_all // 2)], vd.at[0])
    v_arrived(zn - 1, vo.at[0])
    arrived(sums.at[pl.ds(0, n - 1)], su.at[0])
    arrived(means.at[pl.ds(0, zn - 1)], me_sem.at[0])
    for group in range(last + 1):
        arrived(parts.at[pl.ds(0, n - 1), :, group_lanes[group]], rs_sem.at[0, group])
        if len(sym_slots(group)):
            arrived(sym_bytes(group), sy_sem.at[0, group])
        arrived(s_view(group)(pl.ds(0, h - 1), core), ag_sem.at[0, group])
    arrived(t_view(pl.ds(0, h - 1), core), ag_sem.at[0, 3])
    for copy in passes:
        copy.wait_send()
    arrived(yall.at[pl.ds(0, zn - 1)], ya_sem.at[0])
    arrived(tin.at[pl.ds(0, zn - 1)], tz_sem.at[0])


def local(features, grad_out, eigvecs, eigvals, whiten):
    tok, own = features.shape
    n, zn = lax.axis_size("rows"), lax.axis_size("feat")
    d_all = eigvals.shape[0]
    nar, rp = d_all // n, own // n
    h, half = n // 2, zn // 2
    row_count = tok * n
    scratch = [
        pltpu.VMEM((tok, own), bf16),
        pltpu.VMEM((tok, own), bf16),
        pltpu.VMEM((nar, own), f32),
        pltpu.VMEM((1, d_all), f32),
        pltpu.VMEM((d_all, own), bf16),
        pltpu.VMEM((zn, tok, own), bf16),
        pltpu.VMEM((zn, tok, own), bf16),
        pltpu.VMEM((zn, tok, own), bf16),
        pltpu.VMEM((d_all, d_all), bf16),
        pltpu.VMEM((d_all, 2 * nar), bf16),
        pltpu.VMEM((2, nar, own), bf16),
        pltpu.VMEM((own, tok), bf16),
        pltpu.VMEM((tok, own), bf16),
        pltpu.VMEM((tok, own), f32),
        pltpu.VMEM((n, 2, own), f32),
        pltpu.VMEM((2, own), f32),
        pltpu.VMEM((zn, 2, own), f32),
        pltpu.VMEM((n, rp, d_all), bf16),
        pltpu.VMEM((n, rp, d_all), bf16),
        pltpu.VMEM((zn, rp, own), bf16),
        pltpu.VMEM((zn, rp, own), bf16),
        pltpu.VMEM((rp, d_all), bf16),
        pltpu.VMEM((h, 2, rp, d_all), bf16),
        pltpu.VMEM((2 * nar, d_all), bf16),
        pltpu.VMEM((nar, own), f32),
        pltpu.VMEM((zn, nar // zn, own), bf16),
        pltpu.VMEM((zn, nar // zn, own), bf16),
        pltpu.VMEM((nar // zn, d_all), f32),
        pltpu.VMEM((nar // zn, d_all), bf16),
        pltpu.VMEM((zn, nar // zn, own), bf16),
        pltpu.VMEM((zn, nar // zn, own), bf16),
        pltpu.VMEM((nar, own), bf16),
        pltpu.VMEM((h, 2, nar, own), bf16),
        pltpu.VMEM((own, own), bf16),
        pltpu.VMEM((tok, d_all), f32),
        pltpu.VMEM((tok, d_all), bf16),
    ]
    dma = pltpu.SemaphoreType.DMA
    scratch += [dma((5,)), dma((2,)), dma((2, half, CHUNKS[0])), dma((2, half, CHUNKS[1])), dma((1,)), dma((2, half)), dma((2,))]
    scratch += [dma((1,)), dma((zn,)), dma((1,)), dma((zn,)), dma((2,)), dma((2,)), dma((2,)), dma((2,))]
    scratch += [dma((2, 3)), dma((2, 3)), dma((2, 4)), dma((2, 4)), dma((2,)), dma((2,))]
    hbm = pl.BlockSpec(memory_space=pl.ANY)
    return pl.pallas_call(
        functools.partial(body, n, zn, row_count),
        out_shape=pltpu.VMEM((tok, own), bf16),
        in_specs=[hbm] * 5,
        out_specs=VMEM,
        scratch_shapes=scratch,
        compiler_params=pltpu.CompilerParams(collective_id=1, has_side_effects=True, vmem_limit_bytes=58 * 2**20),
        cost_estimate=pl.CostEstimate(flops=8_000_000_000, bytes_accessed=16 * 2**20, transcendentals=0),
    )(features, grad_out, eigvecs.T, eigvals.reshape(1, d_all), whiten)


def solution(mesh):
    in_specs = (P("rows", "feat"), P("rows", "feat"), P("feat", "rows"), P(), P(None, "feat"))
    out_specs = P("rows", "feat")
    return jax.shard_map(local, mesh=mesh, in_specs=in_specs, out_specs=out_specs, check_vma=False)
```

```python
import functools
import math

import jax
import jax.numpy as jnp
from jax import lax
from jax.experimental import pallas as pl
from jax.experimental.pallas import tpu as pltpu
from jax.sharding import PartitionSpec as P

MESH = pl.DeviceIdType.MESH
VMEM = pl.BlockSpec(memory_space=pltpu.VMEM)
bf16, f32 = jnp.bfloat16, jnp.float32
CHUNKS = (4, 4)


def remote(src, dst, send, recv, axis, target):
    return pltpu.make_async_remote_copy(
        src_ref=src, dst_ref=dst, send_sem=send, recv_sem=recv,
        device_id={axis: target}, device_id_type=MESH,
    )


def lanes(index, width):
    return pl.ds(pl.multiple_of(index * width, width), width)


def mm(a, b, ca=1, cb=0):
    return lax.dot_general(a, b, (((ca,), (cb,)), ((), ())), preferred_element_type=f32)


def slot_order(zn):
    order = [0]
    for dist in range(1, zn // 2):
        order += [zn - dist, dist]
    return order + [zn // 2]


def body(n, zn, row_count, x_hbm, g_hbm, v_hbm, e_hbm, w_hbm, o_ref,
         x_ref, g_ref, v_ref, e_ref, w_ref, x_all, xc_all, g_all, v_all, v_col, v_pair, xct, gc, acc, sums, sums_own, means,
         pieces, parts, tile, rtile, spiece, sall, vct, yacc, yown, yall, kern, mt, tout, tin, town, tall, sens, xv, xvb,
         ld, ring_s, ring_g, ring_x, vr_s, vr_r, vm, v1_s, v1_r, v2_s, v2_r, vd, vo, su, me_sem, rs_sem, sy_sem, ag_sem, am_sem, ya_sem, tz_sem):
    me, z = lax.axis_index("rows"), lax.axis_index("feat")
    core, chip = lax.rem(me, 2), me // 2
    mate = me + 1 - 2 * core
    h = n // 2
    nx = math.isqrt(h)
    ny = h // nx
    yy, xx = chip // nx, lax.rem(chip, nx)
    half = zn // 2
    tok, own = x_ref.shape
    d_all = v_all.shape[0]
    nar = d_all // n
    wide = 2 * nar
    hv = own // 2
    rp = own // n
    order = slot_order(zn)
    ring_r = (ring_g, ring_x)

    loads = []
    for i, (src, dst) in enumerate([(g_hbm, g_ref), (v_hbm, v_ref), (x_hbm, x_ref), (e_hbm, e_ref), (w_hbm, w_ref)]):
        load = pltpu.make_async_copy(src, dst, ld.at[i])
        load.start()
        loads.append(load)
    barrier = pltpu.get_barrier_semaphore()
    for d in range(1, n):
        pl.semaphore_signal(barrier, inc=1, device_id={"rows": lax.rem(me + d, n)}, device_id_type=MESH)
    for d in range(1, zn):
        pl.semaphore_signal(barrier, inc=1, device_id={"feat": lax.rem(z + d, zn)}, device_id_type=MESH)
    loads[0].wait()
    loads[1].wait()
    v_pair[core] = v_ref[...].astype(bf16)
    pl.semaphore_wait(barrier, n + zn - 2)

    def at_z(rel):
        return lax.rem(z + rel, zn)

    def rows_of(block, count):
        return pl.ds(pl.multiple_of(block * count, count), count)

    def arrived(ref, sem):
        pltpu.make_async_copy(ref, ref, sem).wait()

    def block_of(way, dist):
        return at_z(zn - dist) if way == 0 else at_z(dist)

    def next_of(way):
        return at_z(1) if way == 0 else at_z(zn - 1)

    def units(arr, step):
        return range(CHUNKS[arr] if step < half - 1 else CHUNKS[arr] // 2)

    def hop(arr, way, step, unit):
        full, mine = (g_all, g_ref) if arr == 0 else (x_all, x_ref)
        count = CHUNKS[arr]
        rows = pl.ds((unit + way * (count // 2)) % count * (tok // count), tok // count)
        there = full.at[block_of(way, step), rows]
        src = there if step else mine.at[rows]
        return remote(src, there, ring_s.at[arr], ring_r[arr].at[way, step, unit], "feat", next_of(way))

    def vpart(block, lane):
        return v_all.at[rows_of(2 * block + core, hv), lanes(lane, wide)]

    def v_mine(block):
        return v_col.at[rows_of(2 * block + core, hv)]

    def v_keep(block):
        rows = rows_of(2 * block + core, hv)
        v_all[rows, lanes(chip, wide)] = v_col[rows]

    def v_arrived(count, sem):
        if count * wide > d_all:
            arrived(v_all.at[pl.ds(0, count * wide * hv // d_all)], sem)
        elif count:
            arrived(v_all.at[pl.ds(0, hv), pl.ds(0, count * wide)], sem)

    def vhop(way, step):
        ref = v_mine(block_of(way, step))
        return remote(ref, ref, vr_s.at[0], vr_r.at[way, step], "feat", next_of(way))

    def y_first(rel):
        return rel == 0 or rel > half

    def by_y(d):
        return (lax.rem(yy + d, ny) * nx + xx) * 2 + core

    def by_x(d):
        return (yy * nx + lax.rem(xx + d, nx)) * 2 + core

    def v_first(rel):
        src, ref = v_mine(at_z(rel)), vpart(at_z(rel), chip)
        if rel:
            remote(src, src, vo.at[0], vo.at[1], "rows", mate).start()
        v_keep(at_z(rel))
        for d in range(1, ny if y_first(rel) else nx):
            target = by_y(d) if y_first(rel) else by_x(d)
            remote(src, ref, v1_s.at[0], v1_r.at[rel], "rows", target).start()

    def v_second(rel):
        v_arrived((ny if y_first(rel) else nx) - 1, v1_r.at[rel])
        if y_first(rel):
            for e in range(ny):
                ref = vpart(at_z(rel), lax.rem(yy + ny - e, ny) * nx + xx)
                src = ref if e else v_mine(at_z(rel))
                for d in range(1, nx):
                    remote(src, ref, v2_s.at[0], v2_r.at[rel], "rows", by_x(d)).start()
        else:
            ref = v_all.at[rows_of(2 * at_z(rel) + core, hv), lanes(yy, nx * wide)]
            for d in range(1, ny):
                remote(ref, ref, v2_s.at[0], v2_r.at[rel], "rows", by_y(d)).start()

    def v_third(rel):
        v_arrived(ny * (nx - 1) if y_first(rel) else nx * (ny - 1), v2_r.at[rel])
        ref = v_all.at[rows_of(2 * at_z(rel) + core, hv)]
        remote(ref, ref, vd.at[0], vd.at[1], "rows", mate).start()

    for way in (0, 1):
        hop(0, way, 0, 0).start()
    pair = remote(v_pair.at[core], v_pair.at[core], vm.at[0], vm.at[1], "rows", mate)
    pair.start()
    loads[2].wait()
    sums_own[0:1] = jnp.sum(x_ref[...].astype(f32), axis=0, keepdims=True)
    sums_own[1:2] = jnp.sum(g_ref[...].astype(f32), axis=0, keepdims=True)
    pair.wait_recv()
    both = jnp.concatenate([v_pair[0].astype(f32), v_pair[1].astype(f32)], axis=0)
    v_col[rows_of(z, own)] = both.T.astype(bf16)
    for way in (0, 1):
        if way == 0 or half > 1:
            vhop(way, 0).start()
        for unit in units(0, 0)[1:]:
            hop(0, way, 0, unit).start()
    for d in range(1, n):
        remote(sums_own, sums.at[me], su.at[0], su.at[1], "rows", lax.rem(me + d, n)).start()
    sums[me] = sums_own[...]
    v_first(0)

    loads[3].wait()
    root = jnp.sqrt(e_ref[...])
    shape = (nar // zn, d_all)
    wanted = me * nar + z * (nar // zn) + lax.broadcasted_iota(jnp.int32, shape, 0)
    hit = wanted == lax.broadcasted_iota(jnp.int32, shape, 1)
    root_row = jnp.sum(jnp.where(hit, jnp.broadcast_to(root, shape), 0.0), axis=1, keepdims=True)
    kern[...] = -1.0 / ((root_row * root) * (root_row + root))

    arrived(sums.at[pl.ds(0, n - 1)], su.at[1])
    means[z] = jnp.sum(sums[...], axis=0) / row_count
    for d in range(1, zn):
        remote(means.at[z], means.at[z], me_sem.at[0], me_sem.at[1], "feat", at_z(d)).start()
    xc = x_ref[...].astype(f32) - means[z, 0:1]
    xc_all[z] = xc.astype(bf16)
    xct[...] = xc.T.astype(bf16)
    loads[4].wait()

    def gram(slot):
        rel = order[slot]
        q = at_z(rel)
        src = g_ref if rel == 0 else g_all.at[q]
        gc[...] = (src[...].astype(f32) - means[q, 1:2]).astype(bf16)
        block = mm(xct[...], gc[...])
        lane = pl.ds(slot * own, own)

        def put(value):
            pieces[:, :, lane] = value.reshape(n, rp, own).astype(bf16)

        if rel == 0:
            put(0.5 * (block + block.T))
        else:
            @pl.when(z < q)
            def _():
                put(0.5 * block)

            @pl.when(z > q)
            def _():
                put(0.5 * block.T)

    def product(slot):
        gw = mm(gc[...], w_ref[rows_of(at_z(order[slot]), own)])
        acc[...] = gw if slot == 0 else acc[...] + gw

    split = max(1, zn - 3)
    groups = [(lo, hi) for lo, hi in ((0, split), (split, zn - 1), (zn - 1, zn)) if lo < hi]
    last = len(groups) - 1
    group_lanes = [pl.ds(lo * own, (hi - lo) * own) for lo, hi in groups]

    def rs_start(group):
        lane = group_lanes[group]
        for d in range(1, n):
            s = lax.rem(me + d, n)
            remote(pieces.at[s, :, lane], parts.at[me, :, lane], rs_sem.at[0, group], rs_sem.at[1, group], "rows", s).start()

    def rs_sum(group):
        (lo, hi), lane = groups[group], group_lanes[group]
        arrived(parts.at[pl.ds(0, n - 1), :, lane], rs_sem.at[1, group])
        total = pieces[me, :, lane].astype(f32)
        for d in range(1, n):
            total = total + parts[lax.rem(me + n - d, n), :, lane].astype(f32)
        for slot in range(lo, hi):
            tile[slot] = total[:, (slot - lo) * own:(slot - lo + 1) * own].astype(bf16)

    def sym_slots(group):
        return range(max(1, groups[group][0]), groups[group][1])

    def sym_start(group):
        for slot in sym_slots(group):
            d = order[slot]
            there = rtile.at[order.index((zn - d) % zn)]
            remote(tile.at[slot], there, sy_sem.at[0, group], sy_sem.at[1, group], "feat", at_z(d)).start()

    def sym_bytes(group):
        return rtile.at[pl.ds(sym_slots(group)[0], len(sym_slots(group)))]

    def sym_end(group):
        if len(sym_slots(group)):
            arrived(sym_bytes(group), sy_sem.at[1, group])
        lo, hi = groups[group]
        for slot in range(lo, hi):
            both = tile[slot].astype(f32)
            if slot:
                both = both + rtile[slot].astype(f32)
            spiece[:, pl.ds(slot * own, own)] = both.astype(bf16)

    def gather_start(which, src, view):
        for d in range(1, h):
            there = lax.rem(chip + d, h)
            remote(src, view(chip, core), ag_sem.at[0, which], ag_sem.at[1, which], "rows", 2 * there + core).start()

    def gather_pass(which, view):
        arrived(view(pl.ds(0, h - 1), core), ag_sem.at[1, which])
        mine = view(pl.ds(0, h), core)
        copy = remote(mine, mine, am_sem.at[0, which], am_sem.at[1, which], "rows", mate)
        copy.start()
        return copy

    def s_view(group):
        return lambda chips, side: sall.at[chips, side, :, group_lanes[group]]

    def t_view(chips, side):
        return tall.at[chips, side]

    done = set()

    def take(arr, way, step, unit):
        if (arr, way, step, unit) not in done:
            done.add((arr, way, step, unit))
            hop(arr, way, step, unit).wait_recv()

    forwards = [(step, unit) for step in range(half) for unit in units(1, step)]
    state = {"next": 0}

    def pump(count):
        for _ in range(count):
            if state["next"] < len(forwards):
                step, unit = forwards[state["next"]]
                state["next"] += 1
                for way in (0, 1):
                    if step:
                        take(1, way, step - 1, unit)
                    hop(1, way, step, unit).start()

    def all_in(arr, dist):
        for unit in units(arr, dist - 1):
            for way in (0, 1):
                take(arr, way, dist - 1, unit)

    def center(rel):
        q = at_z(rel)
        xc_all[q] = (x_all[q].astype(f32) - means[q, 0:1]).astype(bf16)

    gram(0)
    if split == 1:
        rs_start(0)
    product(0)
    v_second(0)
    rels = [[0]]
    for dist in range(1, half + 1):
        got = []
        for way in (0, 1):
            if way == 0 or dist < half:
                vhop(way, dist - 1).wait_recv()
                if (way == 0 and dist < half) or (way == 1 and dist < half - 1):
                    vhop(way, dist).start()
                rel = zn - dist if way == 0 else dist
                v_first(rel)
                got.append(rel)
        rels.append(got)
        for unit in units(0, dist - 1):
            for way in (0, 1):
                take(0, way, dist - 1, unit)
                if dist < half and unit in units(0, dist):
                    hop(0, way, dist, unit).start()
            if dist == half - 1 and unit == 1:
                rs_sum(0)
                sym_start(0)
            if dist == half - 1 and unit == 3:
                pump(1)
            if dist == half:
                pump(1 - unit)
            if dist >= 2 and unit == 1:
                for rel in rels[dist - 2]:
                    v_third(rel)
        if dist == 1:
            arrived(means.at[pl.ds(0, zn - 1)], me_sem.at[1])
        mine = [slot for slot in range(zn) if order[slot] in (dist, zn - dist)]
        for slot in mine:
            gram(slot)
            for group in range(last):
                if slot == groups[group][1] - 1:
                    rs_start(group)
            if dist < half:
                product(slot)
        if dist < half - 1:
            for rel in rels[dist]:
                v_second(rel)
    def s_start(group):
        sym_end(group)
        lane = group_lanes[group]
        sall[chip, core, :, lane] = spiece[:, lane]
        gather_start(group, spiece.at[:, lane], s_view(group))

    rs_start(last)
    product(zn - 1)
    if half == 1:
        rs_sum(0)
        sym_start(0)
    s_start(0)
    if half > 1:
        for rel in rels[half - 1]:
            v_second(rel)
    for group in range(1, last):
        rs_sum(group)
        sym_start(group)
    pump(1)
    rs_sum(last)
    sym_start(last)
    pump(1)
    passes = [gather_pass(0, s_view(0))] if last else []
    for group in range(1, last):
        s_start(group)
    pump(1)
    s_start(last)
    for rel in rels[half]:
        v_second(rel)
    pump(2)
    v_arrived(zn - 1, vo.at[1])
    vct[...] = v_col[...].astype(f32).T.astype(bf16)
    yacc[...] = jnp.zeros_like(yacc)

    def y_part(group):
        passes[group].wait_recv()
        lo, hi = groups[group]
        for slot in range(lo, hi):
            q = at_z(order[slot])
            block = sall[:, :, :, pl.ds(slot * own, own)].astype(f32).reshape(own, own).astype(bf16)
            left = vct[rows_of(core, nar), lanes(q, own)]
            if slot == 0:
                yacc[...] += mm(left, block)
            else:
                @pl.when(q < z)
                def _():
                    yacc[...] += mm(left, block)

                @pl.when(q > z)
                def _():
                    yacc[...] += mm(left, block, 1, 1)

    if last:
        y_part(0)
    for group in range(1, last + 1):
        passes.append(gather_pass(group, s_view(group)))
    if not last:
        passes.append(gather_pass(0, s_view(0)))
    pump(0)
    for group in range(1 if last else 0, last + 1):
        y_part(group)
    yown[...] = yacc[...].reshape(zn, nar // zn, own).astype(bf16)
    for d in range(1, zn):
        remote(yown.at[at_z(d)], yall.at[z], ya_sem.at[0], ya_sem.at[1], "feat", at_z(d)).start()
    yall[z] = yown[z]
    for rel in rels[half - 1] + rels[half]:
        v_third(rel)
    pump(1)
    if half > 1:
        all_in(1, 1)
        center(zn - 1)
        center(1)

    def early(rels, first, final):
        rows_each = tok // 4

        @pl.loop(0, 4)
        def _(i):
            rows = rows_of(i, rows_each)
            total = 0.0 if first else xv[rows]
            for rel in rels:
                q = at_z(rel)
                total = total + mm(xc_all[q, rows], v_all[rows_of(q, own)])
            if final:
                xvb[rows] = total.astype(bf16)
            else:
                xv[rows] = total

    arrived(yall.at[pl.ds(0, zn - 1)], ya_sem.at[1])
    pump(1)
    arrived(v_all.at[pl.ds(0, d_all // 2)], vd.at[1])
    left = jnp.concatenate([yall[q] for q in range(zn)], axis=1)
    mt[...] = (kern[...] * mm(left, v_all[...])).astype(bf16)
    t_rows = mm(mt[...], v_all[...], 1, 1)
    for q in range(zn):
        tout[q] = t_rows[:, q * own:(q + 1) * own].astype(bf16)
    for d in range(1, zn):
        remote(tout.at[at_z(d)], tin.at[z], tz_sem.at[0], tz_sem.at[1], "feat", at_z(d)).start()
    tin[z] = tout[z]
    pump(2)
    early([0, zn - 1, 1] if half > 1 else [0], True, half <= 2)
    arrived(tin.at[pl.ds(0, zn - 1)], tz_sem.at[1])
    town[...] = tin[...].astype(f32).reshape(nar, own).astype(bf16)
    tall[chip, core] = town[...]
    gather_start(3, town, t_view)
    pump(2)
    for dist in range(2, half):
        if dist == half - 1:
            passes.append(gather_pass(3, t_view))
        all_in(1, dist)
        center(zn - dist)
        center(dist)
        early([zn - dist, dist] if dist < half - 1 else [zn - dist], False, dist == half - 1)
        pump(1)
    if half <= 2:
        passes.append(gather_pass(3, t_view))
    pump(len(forwards))
    passes[-1].wait_recv()
    scale = 2.0 / row_count
    acc[...] += scale * mm(xvb[...], tall[...].reshape(d_all, own))
    late = [half - 1, half] if half > 2 else [half]
    for i, rel in enumerate(late):
        part = mm(v_all[rows_of(at_z(rel), own)], tall[...].reshape(d_all, own))
        sens[i] = (scale * part).astype(bf16)
    for i, rel in enumerate(late[:-1]):
        acc[...] += mm(xc_all[at_z(rel)], sens[i])
    all_in(1, half)
    center(half)
    o_ref[...] = (acc[...] + mm(xc_all[at_z(half)], sens[len(late) - 1])).astype(bf16)

    pair.wait_send()
    for arr, full in ((0, g_all), (1, x_all)):
        arrived(full.at[pl.ds(0, zn - 1)], ring_s.at[arr])
    v_arrived(zn - 1, vr_s.at[0])
    v_arrived(sum((ny if y_first(rel) else nx) - 1 for rel in range(zn)), v1_s.at[0])
    v_arrived(sum(ny * (nx - 1) if y_first(rel) else nx * (ny - 1) for rel in range(zn)), v2_s.at[0])
    arrived(v_all.at[pl.ds(0, d_all // 2)], vd.at[0])
    v_arrived(zn - 1, vo.at[0])
    arrived(sums.at[pl.ds(0, n - 1)], su.at[0])
    arrived(means.at[pl.ds(0, zn - 1)], me_sem.at[0])
    for group in range(last + 1):
        arrived(parts.at[pl.ds(0, n - 1), :, group_lanes[group]], rs_sem.at[0, group])
        if len(sym_slots(group)):
            arrived(sym_bytes(group), sy_sem.at[0, group])
        arrived(s_view(group)(pl.ds(0, h - 1), core), ag_sem.at[0, group])
    arrived(t_view(pl.ds(0, h - 1), core), ag_sem.at[0, 3])
    for copy in passes:
        copy.wait_send()
    arrived(yall.at[pl.ds(0, zn - 1)], ya_sem.at[0])
    arrived(tin.at[pl.ds(0, zn - 1)], tz_sem.at[0])


def local(features, grad_out, eigvecs, eigvals, whiten):
    tok, own = features.shape
    n, zn = lax.axis_size("rows"), lax.axis_size("feat")
    d_all = eigvals.shape[0]
    nar, rp = d_all // n, own // n
    h, half = n // 2, zn // 2
    row_count = tok * n
    scratch = [
        pltpu.VMEM((tok, own), bf16),
        pltpu.VMEM((tok, own), bf16),
        pltpu.VMEM((nar, own), f32),
        pltpu.VMEM((1, d_all), f32),
        pltpu.VMEM((d_all, own), bf16),
        pltpu.VMEM((zn, tok, own), bf16),
        pltpu.VMEM((zn, tok, own), bf16),
        pltpu.VMEM((zn, tok, own), bf16),
        pltpu.VMEM((d_all, d_all), bf16),
        pltpu.VMEM((d_all, 2 * nar), bf16),
        pltpu.VMEM((2, nar, own), bf16),
        pltpu.VMEM((own, tok), bf16),
        pltpu.VMEM((tok, own), bf16),
        pltpu.VMEM((tok, own), f32),
        pltpu.VMEM((n, 2, own), f32),
        pltpu.VMEM((2, own), f32),
        pltpu.VMEM((zn, 2, own), f32),
        pltpu.VMEM((n, rp, d_all), bf16),
        pltpu.VMEM((n, rp, d_all), bf16),
        pltpu.VMEM((zn, rp, own), bf16),
        pltpu.VMEM((zn, rp, own), bf16),
        pltpu.VMEM((rp, d_all), bf16),
        pltpu.VMEM((h, 2, rp, d_all), bf16),
        pltpu.VMEM((2 * nar, d_all), bf16),
        pltpu.VMEM((nar, own), f32),
        pltpu.VMEM((zn, nar // zn, own), bf16),
        pltpu.VMEM((zn, nar // zn, own), bf16),
        pltpu.VMEM((nar // zn, d_all), f32),
        pltpu.VMEM((nar // zn, d_all), bf16),
        pltpu.VMEM((zn, nar // zn, own), bf16),
        pltpu.VMEM((zn, nar // zn, own), bf16),
        pltpu.VMEM((nar, own), bf16),
        pltpu.VMEM((h, 2, nar, own), bf16),
        pltpu.VMEM((2, own, own), bf16),
        pltpu.VMEM((tok, d_all), f32),
        pltpu.VMEM((tok, d_all), bf16),
    ]
    dma = pltpu.SemaphoreType.DMA
    scratch += [dma((5,)), dma((2,)), dma((2, half, CHUNKS[0])), dma((2, half, CHUNKS[1])), dma((1,)), dma((2, half)), dma((2,))]
    scratch += [dma((1,)), dma((zn,)), dma((1,)), dma((zn,)), dma((2,)), dma((2,)), dma((2,)), dma((2,))]
    scratch += [dma((2, 3)), dma((2, 3)), dma((2, 4)), dma((2, 4)), dma((2,)), dma((2,))]
    hbm = pl.BlockSpec(memory_space=pl.ANY)
    return pl.pallas_call(
        functools.partial(body, n, zn, row_count),
        out_shape=pltpu.VMEM((tok, own), bf16),
        in_specs=[hbm] * 5,
        out_specs=VMEM,
        scratch_shapes=scratch,
        compiler_params=pltpu.CompilerParams(collective_id=1, has_side_effects=True, vmem_limit_bytes=58 * 2**20),
        cost_estimate=pl.CostEstimate(flops=8_000_000_000, bytes_accessed=16 * 2**20, transcendentals=0),
    )(features, grad_out, eigvecs.T, eigvals.reshape(1, d_all), whiten)


def solution(mesh):
    in_specs = (P("rows", "feat"), P("rows", "feat"), P("feat", "rows"), P(), P(None, "feat"))
    out_specs = P("rows", "feat")
    return jax.shard_map(local, mesh=mesh, in_specs=in_specs, out_specs=out_specs, check_vma=False)
```
